8 devices in a mesh: rep: 1 (over z), dp: 8 (over x, y, core).
Axes of the slice: x: 2, y: 2, z: 1, core: 2. Of those that a mesh axis runs over, the one named last changes fastest.
Arguments:
- x: bfloat16 [8, 2048, 512], P(('rep', 'dp'))
- dy: bfloat16 [8, 2048, 512], P(('rep', 'dp'))
- wq: bfloat16 [2, 512, 2048], replicated
- wk: bfloat16 [2, 512, 2048], replicated
- wv: bfloat16 [2, 512, 2048], replicated
- wo: bfloat16 [2, 2048, 512], replicated
- w_gate: bfloat16 [2, 512, 8192], replicated
- w_up: bfloat16 [2, 512, 8192], replicated
- w_down: bfloat16 [2, 8192, 512], replicated
- m_wq: float32 [2, 512, 2048], P(None, 'dp')
- m_wk: float32 [2, 512, 2048], P(None, 'dp')
- m_wv: float32 [2, 512, 2048], P(None, 'dp')
- m_wo: float32 [2, 2048, 512], P(None, 'dp')
- m_w_gate: float32 [2, 512, 8192], P(None, 'dp')
- m_w_up: float32 [2, 512, 8192], P(None, 'dp')
- m_w_down: float32 [2, 8192, 512], P(None, 'dp')
- v_wq: float32 [2, 512, 2048], P(None, 'dp')
- v_wk: float32 [2, 512, 2048], P(None, 'dp')
- v_wv: float32 [2, 512, 2048], P(None, 'dp')
- v_wo: float32 [2, 2048, 512], P(None, 'dp')
- v_w_gate: float32 [2, 512, 8192], P(None, 'dp')
- v_w_up: float32 [2, 512, 8192], P(None, 'dp')
- v_w_down: float32 [2, 8192, 512], P(None, 'dp')
Outputs:
- output 1: bfloat16 [2, 512, 2048], P('rep')
- output 2: bfloat16 [2, 512, 2048], P('rep')
- output 3: bfloat16 [2, 512, 2048], P('rep')
- output 4: bfloat16 [2, 2048, 512], P('rep')
- output 5: bfloat16 [2, 512, 8192], P('rep')
- output 6: bfloat16 [2, 512, 8192], P('rep')
- output 7: bfloat16 [2, 8192, 512], P('rep')
- output 8: float32 [2, 512, 2048], P('rep', 'dp')
- output 9: float32 [2, 512, 2048], P('rep', 'dp')
- output 10: float32 [2, 512, 2048], P('rep', 'dp')
- output 11: float32 [2, 2048, 512], P('rep', 'dp')
- output 12: float32 [2, 512, 8192], P('rep', 'dp')
- output 13: float32 [2, 512, 8192], P('rep', 'dp')
- output 14: float32 [2, 8192, 512], P('rep', 'dp')
- output 15: float32 [2, 512, 2048], P('rep', 'dp')
- output 16: float32 [2, 512, 2048], P('rep', 'dp')
- output 17: float32 [2, 512, 2048], P('rep', 'dp')
- output 18: float32 [2, 2048, 512], P('rep', 'dp')
- output 19: float32 [2, 512, 8192], P('rep', 'dp')
- output 20: float32 [2, 512, 8192], P('rep', 'dp')
- output 21: float32 [2, 8192, 512], P('rep', 'dp')
All inputs are finite; a program needn't handle non-finite values.
Results may differ from the reference program's by a relative error of at most 0.024.
Values are sent between devices in bfloat16 or wider.
A program may use at most 2 GiB of HBM per device.

```python
import jax
import jax.numpy as jnp
from jax import lax

SEQUENCES = 8
TOKENS = 2048
D = 512
HEADS = 16
KV_HEADS = 16
HEAD = 128
FF = 8192
LAYERS = 2
THETA = 10000
NAMES = ("wq", "wk", "wv", "wo", "w_gate", "w_up", "w_down")
SHAPES = {
    "wq": (LAYERS, D, HEADS * HEAD),
    "wk": (LAYERS, D, KV_HEADS * HEAD),
    "wv": (LAYERS, D, KV_HEADS * HEAD),
    "wo": (LAYERS, HEADS * HEAD, D),
    "w_gate": (LAYERS, D, FF),
    "w_up": (LAYERS, D, FF),
    "w_down": (LAYERS, FF, D),
}


def bump(key, n, height):
    away = (jnp.arange(n, dtype=jnp.int32) - jax.random.randint(key, (), 0, n, jnp.int32)) % n
    return jnp.where(away < n // 8, height, 1.0)


def together(key, own, strength):
    shared = jax.random.normal(key, own.shape[1:], jnp.float32)
    return (own + strength * shared) * lax.rsqrt(1 + strength * strength)


def setup_inputs(seed: int = 0, part: int = 0) -> dict:
    kx, kdy, ka, kb, kz, kf, kh, kl, *keys = jax.random.split(jax.random.key(seed), 8 + 3 * len(NAMES))
    kx, kdy, ka, kb = (jax.random.fold_in(k, part) for k in (kx, kdy, ka, kb))
    kw, km, kv = (keys[i::3] for i in range(3))
    shape = (SEQUENCES, TOKENS, D)
    much_x, much_dy = jax.random.uniform(kz, (2,), jnp.float32, 0.0, 1.0)
    loud = 2.0 ** jax.random.uniform(jax.random.fold_in(kz, 1), (), jnp.float32, -1.0, 2.0)
    layers = 2.0 ** jax.random.uniform(kl, (LAYERS, 1, 1), jnp.float32, -1.0, 1.0)
    times = {"wq": 1.0, "wk": 1.0, "wv": 2.0, "wo": layers, "w_gate": 1.0, "w_up": bump(kh, FF, 4.0), "w_down": layers}
    x = together(ka, jax.random.normal(kx, shape, jnp.float32), much_x) * bump(kf, D, 4.0)
    dy = together(kb, jax.random.normal(kdy, shape, jnp.float32), much_dy)
    drawn = {"x": x.astype(jnp.bfloat16), "dy": (loud * dy * (SEQUENCES * TOKENS) ** -0.5).astype(jnp.bfloat16)}
    for key, name in zip(kw, NAMES, strict=True):
        drawn[name] = (jax.random.normal(key, SHAPES[name], jnp.float32) * SHAPES[name][1] ** -0.5 * times[name]).astype(jnp.bfloat16)
    for key, name in zip(km, NAMES, strict=True):
        drawn[f"m_{name}"] = 0.1 * jax.random.normal(key, SHAPES[name], jnp.float32)
    for key, name in zip(kv, NAMES, strict=True):
        drawn[f"v_{name}"] = loud * loud * jax.random.uniform(key, SHAPES[name], jnp.float32, 0.2, 0.6)
    return drawn


def matmul(a, w):
    return jnp.dot(a, w, preferred_element_type=jnp.float32).astype(jnp.bfloat16)


def normed(h):
    wide = h.astype(jnp.float32)
    scale = lax.rsqrt(jnp.mean(wide**2, -1, keepdims=True) + 1e-6)
    return (wide * scale).astype(jnp.bfloat16)


def turned(t, theta):
    half = t.shape[-1] // 2
    angle = jnp.arange(t.shape[0], dtype=jnp.float32)[:, None] * theta ** (-jnp.arange(half, dtype=jnp.float32) / half)
    cos, sin = jnp.cos(angle)[:, None], jnp.sin(angle)[:, None]
    a, b = t[..., :half].astype(jnp.float32), t[..., half:].astype(jnp.float32)
    return jnp.concatenate([a * cos - b * sin, b * cos + a * sin], -1).astype(jnp.bfloat16)


def seen_by(q, k, v):
    tokens, kv = q.shape[0], k.shape[1]
    q = q.reshape(tokens, kv, -1, q.shape[-1])
    scores = jnp.einsum("tgsd,ugd->gstu", q.astype(jnp.float32), k.astype(jnp.float32)) * q.shape[-1] ** -0.5
    place = jnp.arange(tokens)
    weights = jax.nn.softmax(jnp.where(place[:, None] >= place, scores, -jnp.inf), -1).astype(jnp.bfloat16)
    return jnp.einsum("gstu,ugd->tgsd", weights.astype(jnp.float32), v.astype(jnp.float32)).astype(jnp.bfloat16).reshape(tokens, -1)


def layer(h, w):
    a = normed(h)
    q, k = (turned(matmul(a, w[name]).reshape(h.shape[0], -1, HEAD), THETA) for name in ("wq", "wk"))
    h = h + matmul(seen_by(q, k, matmul(a, w["wv"]).reshape(h.shape[0], -1, HEAD)), w["wo"])
    b = normed(h)
    gate = jnp.dot(b, w["w_gate"], preferred_element_type=jnp.float32)
    up = jnp.dot(b, w["w_up"], preferred_element_type=jnp.float32)
    return h + matmul((jax.nn.silu(gate) * up).astype(jnp.bfloat16), w["w_down"])


def adamw(w, m, v, g):
    m = 0.9 * m + 0.1 * g
    v = 0.95 * v + 0.05 * g * g
    step = m * lax.rsqrt(v + 1e-8) + 0.1 * w
    return (w - 0.02 * step).astype(jnp.bfloat16), m, v


def stack(weights, h):
    return lax.scan(lambda h, w: (layer(h, w), None), h, weights)[0]


def reference(x, dy, wq, wk, wv, wo, w_gate, w_up, w_down, m_wq, m_wk, m_wv, m_wo, m_w_gate, m_w_up, m_w_down, v_wq, v_wk, v_wv, v_wo, v_w_gate, v_w_up, v_w_down):
    weights = dict(zip(NAMES, (wq, wk, wv, wo, w_gate, w_up, w_down), strict=True))

    def take(so_far, sequence):
        h, by_y = sequence
        _, back = jax.vjp(stack, weights, h)
        by_weights, by_h = back(by_y)
        return jax.tree.map(lambda total, term: total + term.astype(jnp.float32), so_far, by_weights), by_h

    none_yet = {name: jnp.zeros(w.shape, jnp.float32) for name, w in weights.items()}
    by_weights, by_x = lax.scan(take, none_yet, (x, dy))
    gradients = [by_weights[name].astype(jnp.bfloat16).astype(jnp.float32) for name in NAMES]
    first = (m_wq, m_wk, m_wv, m_wo, m_w_gate, m_w_up, m_w_down)
    second = (v_wq, v_wk, v_wv, v_wo, v_w_gate, v_w_up, v_w_down)
    new = [adamw(weights[name].astype(jnp.float32), m, v, g) for name, m, v, g in zip(NAMES, first, second, gradients, strict=True)]
    return tuple(one[which] for which in range(3) for one in new)
```

```python
import functools

import jax
import jax.numpy as jnp
from jax import lax
from jax.experimental import pallas as pl
from jax.experimental.pallas import tpu as pltpu
from jax.sharding import PartitionSpec as P

T, D, FF, H, HD = 2048, 512, 8192, 16, 128
N = 8
HH = H * HD
PAIR = 2 * HD
BLK = D // N
CH = FF // N
TILE = 256
KEYS = 512
STEPS = 3
SCALE = HD**-0.5
EXP = SCALE * 1.4426950408889634
EPS = 1e-6
VMEM = 63 * 2**20
f32, bf16 = jnp.float32, jnp.bfloat16
MESH = pl.DeviceIdType.MESH
ONE = pl.Buffered(1)
HBM = pl.BlockSpec(memory_space=pl.ANY)


def dot(a, b):
    return lax.dot_general(a, b, (((1,), (0,)), ((), ())), preferred_element_type=f32)


def dot_t(a, b):
    return lax.dot_general(a, b, (((1,), (1,)), ((), ())), preferred_element_type=f32)


def part(n, size, base=0):
    return slice(base + n * size, base + n * size + size)


def loop(count, size, body):
    lax.fori_loop(0, count, lambda t, _: body(pl.ds(pl.multiple_of(t * size, size), size)), None)


def at_step(n):
    return pl.when(pl.program_id(0) == n)


def normed(h):
    wide = h.astype(f32)
    return (wide * lax.rsqrt(jnp.mean(wide * wide, -1, keepdims=True) + EPS)).astype(bf16)


def normed_back(h, by):
    wide, by = h.astype(f32), by.astype(bf16).astype(f32)
    scale = lax.rsqrt(jnp.mean(wide * wide, -1, keepdims=True) + EPS)
    return (by * scale - wide * (scale * scale * scale * jnp.mean(by * wide, -1, keepdims=True))).astype(bf16)


def turned(x, c, s):
    return (x * c + pltpu.roll(x, HD // 2, 1) * s).astype(bf16)


def turned_back(x, c, s):
    return (x * c - pltpu.roll(x, HD // 2, 1) * s).astype(bf16)


def tables():
    half = HD // 2
    angle = jnp.arange(T, dtype=f32)[:, None] * 10000 ** (-jnp.arange(half, dtype=f32) / half)
    c, s = jnp.cos(angle), jnp.sin(angle)
    return jnp.concatenate([c, c], 1), jnp.concatenate([-s, s], 1)


def whole(*shape):
    return pl.BlockSpec(shape, lambda *_: (0,) * len(shape), pipeline_mode=ONE)


def shape(dims, dtype=bf16):
    return jax.ShapeDtypeStruct(dims, dtype)


def params(**more):
    return pltpu.CompilerParams(dimension_semantics=("arbitrary",), vmem_limit_bytes=VMEM, **more)


def cost(flops, exps, moved):
    return pl.CostEstimate(flops=flops, transcendentals=exps, bytes_accessed=moved)


def attn_fwd_kernel(h_ref, wq_ref, wk_ref, wv_ref, wo_ref, c_ref, s_ref, q_ref, k_ref, v_ref, o_ref, lse_ref, h1_ref, a_s, acc_s, vt_s):
    @at_step(0)
    def _():
        def start(rows):
            a_s[rows, :] = normed(h_ref[rows, :])
            acc_s[rows, :] = jnp.zeros((TILE, D), f32)

        loop(T // TILE, TILE, start)
        vt_s[:, HD:, :] = jnp.ones((2, N, T), bf16)

    wq, wk, wv = wq_ref[0], wk_ref[0], wv_ref[0]
    for t in range(T // KEYS):
        rows = part(t, KEYS)
        a = a_s[rows, :]
        v = dot(a, wv).astype(bf16)
        v_ref[rows, :] = v
        for n in range(2):
            vt_s[n, :HD, rows] = v[:, part(n, HD)].T
        for w, ref in ((wq, q_ref), (wk, k_ref)):
            x = dot(a, w).astype(bf16).astype(f32)
            for n in range(2):
                ref[rows, part(n, HD)] = turned(x[:, part(n, HD)], c_ref[rows, :], s_ref[rows, :])

    tile = (TILE, TILE)
    seen = lax.broadcasted_iota(jnp.int32, tile, 1) >= lax.broadcasted_iota(jnp.int32, tile, 0)

    def scores(n, i):
        cols, rows = part(n, HD), part(i, TILE)
        q = q_ref[rows, cols]
        end = i * TILE
        out = [(a, dot_t(k_ref[a : min(a + KEYS, end), cols], q)) for a in range(0, end, KEYS)]
        return out + [(end, jnp.where(seen, dot_t(k_ref[rows, cols], q), -1e30))]

    def finish(n, i, pieces):
        rows = part(i, TILE)
        top = functools.reduce(jnp.maximum, [s.max(0, keepdims=True) for _, s in pieces])
        mix = sum(dot(vt_s[n, :, a : a + s.shape[0]], jnp.exp2((s - top) * EXP).astype(bf16)) for a, s in pieces)
        total = mix[HD : HD + 1]
        o_ref[rows, part(n, HD)] = (mix[:HD] * (1 / total)).T.astype(bf16)
        lse_ref[0, n : n + 1, rows] = top * SCALE + jnp.log(total)

    todo = [(n, i) for i in range(T // TILE) for n in range(2)]
    ready = [scores(*one) for one in todo[:2]]
    for z, one in enumerate(todo):
        ready += [scores(*two) for two in todo[z + 2 : z + STEPS]]
        finish(*one, ready[z])

    acc_s[...] += dot(o_ref[...], wo_ref[0])

    @at_step(N - 1)
    def _():
        def end(rows):
            h1_ref[rows, :] = h_ref[rows, :] + acc_s[rows, :].astype(bf16)

        loop(T // TILE, TILE, end)


def attn_fwd(h, wq, wk, wv, wo, c, s, layer):
    win = pl.BlockSpec((1, D, PAIR), lambda i: (layer, 0, i))
    col = pl.BlockSpec((T, PAIR), lambda i: (0, i))
    return pl.pallas_call(
        attn_fwd_kernel,
        grid=(N,),
        in_specs=[whole(T, D), win, win, win, pl.BlockSpec((1, PAIR, D), lambda i: (layer, i, 0)), whole(T, HD), whole(T, HD)],
        out_specs=[col] * 4 + [pl.BlockSpec((1, 2, T), lambda i: (i, 0, 0)), whole(T, D)],
        out_shape=[shape((T, HH))] * 4 + [shape((N, 2, T), f32), shape((T, D))],
        scratch_shapes=[pltpu.VMEM((T, D), bf16), pltpu.VMEM((T, D), f32), pltpu.VMEM((2, HD + N, T), bf16)],
        compiler_params=params(),
        cost_estimate=cost(N * T * D * HH + 2 * T * T * HH, T * T * N, N * T * HH),
        name="attn_fwd",
    )(h, wq, wk, wv, wo, c, s)


def mlp_fwd_kernel(h1_ref, wg_ref, wu_ref, wd_ref, h2_ref, b_s, acc_s):
    @at_step(0)
    def _():
        def start(rows):
            b_s[rows, :] = normed(h1_ref[rows, :])
            acc_s[rows, :] = jnp.zeros((TILE, D), f32)

        loop(T // TILE, TILE, start)

    wg, wu, wd = wg_ref[0], wu_ref[0], wd_ref[0]
    for t in range(T // TILE):
        rows = part(t, TILE)
        b = b_s[rows, :]
        gate, up = dot(b, wg), dot(b, wu)
        acc_s[rows, :] += dot((gate / (1 + jnp.exp(-gate)) * up).astype(bf16), wd)

    @at_step(N - 1)
    def _():
        def end(rows):
            h2_ref[rows, :] = h1_ref[rows, :] + acc_s[rows, :].astype(bf16)

        loop(T // TILE, TILE, end)


def mlp_fwd(h1, wg, wu, wd, layer):
    win = pl.BlockSpec((1, D, CH), lambda f: (layer, 0, f))
    return pl.pallas_call(
        mlp_fwd_kernel,
        grid=(N,),
        in_specs=[whole(T, D), win, win, pl.BlockSpec((1, CH, D), lambda f: (layer, f, 0))],
        out_specs=whole(T, D),
        out_shape=shape((T, D)),
        scratch_shapes=[pltpu.VMEM((T, D), bf16), pltpu.VMEM((T, D), f32)],
        compiler_params=params(),
        cost_estimate=cost(6 * T * D * FF, T * FF, 6 * D * FF),
        name="mlp_fwd",
    )(h1, wg, wu, wd)


class Reduce:
    @staticmethod
    def scratch(rows, cols):
        half = (rows, cols // 2)
        return [
            pltpu.VMEM((4, 2, rows, cols), bf16),
            pltpu.VMEM((2, 4, rows, cols), bf16),
            pltpu.VMEM((2, 2, *half), bf16),
            pltpu.VMEM((2, 2, *half), f32),
            pltpu.VMEM((2, 2, 2, *half), bf16),
            pltpu.VMEM((2, *half), bf16),
            pltpu.VMEM((2, *half), f32),
            pltpu.VMEM((2, 2, *half), bf16),
            pltpu.SemaphoreType.DMA((5,)),
            pltpu.SemaphoreType.DMA((2, 5)),
        ]

    def __init__(self, refs):
        self.g, self.r1, self.s2, self.k2, self.r2, self.s3, self.k3, self.r3, self.sent, self.came = refs
        self.rows, self.half = self.s3.shape[1], self.s3.shape[2]
        rep, me = lax.axis_index("rep"), lax.axis_index("dp")
        self.x, self.y, self.c = lax.div(me, 4), lax.rem(lax.div(me, 2), 2), lax.rem(me, 2)
        to = lambda x, y, c: (rep, 4 * x + 2 * y + c)
        self.core = to(self.x, self.y, 1 - self.c)
        self.along = to(1 - self.x, self.y, self.c), to(self.x, 1 - self.y, self.c)

    def enter(self):
        barrier = pltpu.get_barrier_semaphore()
        for one in (self.core, *self.along):
            pl.semaphore_signal(barrier, inc=1, device_id=one, device_id_type=MESH)
        pl.semaphore_wait(barrier, STEPS)

    def copy(self, src, dst, slot, k, device):
        return pltpu.make_async_remote_copy(src, dst, self.sent.at[k], self.came.at[slot, k], device_id=device, device_id_type=MESH)

    def copy1(self, n):
        s = lax.rem(n, 2)
        return self.copy(self.g.at[:, 1 - self.c], self.r1.at[s], s, 0, self.core)

    def copy2(self, n, w):
        s = lax.rem(n, 2)
        return self.copy(self.s2.at[w], self.r2.at[s, w], s, 1 + w, self.along[w])

    def copy3(self, n, w):
        s = lax.rem(n, 2)
        return self.copy(self.s3.at[w], self.r3.at[s, w], s, STEPS + w, self.along[1 - w])

    def run(self, body):
        loop(self.rows // BLK, BLK, body)

    def first(self, n):
        s = lax.rem(n, 2)
        self.copy1(n).wait()
        for w in range(2):
            cols = part(w, self.half)
            for o in range(2):
                away = (2 * (1 - self.x) + o, 2 * o + 1 - self.y)[w]
                near = (2 * self.x + o, 2 * o + self.y)[w]

                def go(r):
                    both = lambda b: self.g[b, self.c, r, cols].astype(f32) + self.r1[s, b, r, cols].astype(f32)
                    self.s2[w, o, r, :] = both(away).astype(bf16)
                    self.k2[w, o, r, :] = both(near)

                self.run(go)
            self.copy2(n, w).start()

    def second(self, n):
        s = lax.rem(n, 2)
        for w in range(2):
            mine = (self.y, self.x)[w]
            self.copy2(n, w).wait()

            def go(r):
                both = lambda b: self.k2[w, b, r, :] + self.r2[s, w, b, r, :].astype(f32)
                self.s3[w, r, :] = both(1 - mine).astype(bf16)
                self.k3[w, r, :] = both(mine)

            self.run(go)
            self.copy3(n, w).start()

    def last(self, n, out_ref):
        s = lax.rem(n, 2)
        for w in range(2):
            self.copy3(n, w).wait()

            def go(r):
                out_ref[0, r, part(w, self.half)] = (self.k3[w, r, :] + self.r3[s, w, r, :].astype(f32)).astype(bf16)

            self.run(go)

    def point(self, f, out_ref):
        for late, stage in ((3, lambda n: self.last(n, out_ref)), (2, self.second), (1, self.first)):
            pl.when((f >= late) & (f < N + late))(functools.partial(stage, f - late))

    def send(self, f):
        self.copy1(f).start()


def mlp_bwd_kernel(*refs):
    h1_ref, dh_ref = refs[:2]
    wgs, wus, refs = refs[2 : 2 + N], refs[2 + N : 2 + 2 * N], refs[2 + 2 * N :]
    wd_ref, sum_ref, dh1_ref, b_s, bt_s, dht_s, db_s, act_s, dg_s, du_s = refs[:10]
    red = Reduce(refs[10:])
    f = pl.program_id(0)

    @at_step(0)
    def _():
        red.enter()

        def start(rows):
            b = normed(h1_ref[rows, :])
            b_s[rows, :] = b
            bt_s[:, rows] = b.T
            dht_s[:, rows] = dh_ref[rows, :].T
            db_s[rows, :] = jnp.zeros((TILE, D), f32)

        loop(T // TILE, TILE, start)

    joined = lambda pieces: jnp.concatenate([p[0] for p in pieces], axis=1)

    @pl.when(f < N)
    def _():
        wg, wu, wd = joined(wgs), joined(wus), wd_ref[0].reshape(CH, D)
        for t in range(T // TILE):
            rows = part(t, TILE)
            b = b_s[rows, :]
            gate, up, dact = dot(b, wg), dot(b, wu), dot_t(dh_ref[rows, :], wd).astype(bf16).astype(f32)
            sig = 1 / (1 + jnp.exp(-gate))
            silu = gate * sig
            act_s[rows, :] = (silu * up).astype(bf16)
            du_s[rows, :] = (dact * silu).astype(bf16)
            dg_s[rows, :] = (dact * up * (sig + silu * (1 - sig))).astype(bf16)

    red.point(f, sum_ref)

    @pl.when(f < N)
    def _():
        for n, ref in enumerate((dg_s, du_s)):
            red.g[:, :, part(n, BLK), :] = dot(bt_s[...], ref[...]).astype(bf16).reshape(4, 2, BLK, CH)
        down = dot(dht_s[...], act_s[...]).astype(bf16).T.reshape(4, 2, HD, D)
        for k in range(2):
            red.g[:, :, part(2, BLK), part(k, D)] = down[:, :, part(k, BLK)]
        red.send(f)
        db_s[...] += dot_t(dg_s[...], joined(wgs)) + dot_t(du_s[...], joined(wus))

    @at_step(N - 1)
    def _():
        def end(rows):
            dh1_ref[rows, :] = dh_ref[rows, :] + normed_back(h1_ref[rows, :], db_s[rows, :])

        loop(T // TILE, TILE, end)


def clamped(i):
    return jnp.minimum(i, N - 1)


def summed(i):
    return jnp.maximum(i - STEPS, 0)


def mlp_bwd(h1, dh, wg, wu, wd, layer):
    rows = STEPS * BLK
    cols = [pl.BlockSpec((1, D, HD), functools.partial(lambda d, f: (layer, 0, d * N + clamped(f)), d)) for d in range(N)]
    return pl.pallas_call(
        mlp_bwd_kernel,
        grid=(N + STEPS,),
        in_specs=[whole(T, D), whole(T, D)] + cols * 2 + [pl.BlockSpec((1, N, HD, D), lambda f: (layer, 0, clamped(f), 0))],
        out_specs=[pl.BlockSpec((1, rows, CH), lambda f: (summed(f), 0, 0)), whole(T, D)],
        out_shape=[shape((N, rows, CH)), shape((T, D))],
        scratch_shapes=[pltpu.VMEM((T, D), bf16), pltpu.VMEM((D, T), bf16), pltpu.VMEM((D, T), bf16), pltpu.VMEM((T, D), f32)]
        + [pltpu.VMEM((T, CH), bf16)] * 3
        + Reduce.scratch(rows, CH),
        compiler_params=params(collective_id=1 + layer, has_side_effects=True),
        cost_estimate=cost(16 * T * D * FF, T * FF, 12 * D * FF),
        name="mlp_bwd",
    )(h1, dh, *[wg] * N, *[wu] * N, wd.reshape(2, N, CH, D))


def attn_bwd_kernel(*refs, need_dh):
    h_ref, dh1_ref, q_ref, k_ref, v_ref, o_ref, lse_ref, wo_ref, c_ref, s_ref = refs[:10]
    refs = refs[10:]
    if need_dh:
        ws, sum_ref, dh_ref, da_s, refs = refs[:3], *refs[3:6], refs[6:]
    else:
        sum_ref, refs = refs[0], refs[1:]
    at_s, do_s, dq_s, dk_s, dv_s, qt_s, dot_s, acc_s, lse_s, delta_s, gwo_s = refs[:11]
    red = Reduce(refs[11:])
    f = pl.program_id(0)

    @at_step(0)
    def _():
        red.enter()

        def start(rows):
            at_s[:, rows] = normed(h_ref[rows, :]).T
            if need_dh:
                da_s[rows, :] = jnp.zeros((TILE, D), f32)

        loop(T // TILE, TILE, start)

        def outer(r, _):
            gwo_s[r] = dot(o_ref[:, pl.ds(pl.multiple_of(r * PAIR, PAIR), PAIR)].T, dh1_ref[...]).astype(bf16)

        lax.fori_loop(0, N, outer, None)

    tile = (TILE, TILE)
    seen = lax.broadcasted_iota(jnp.int32, tile, 0) >= lax.broadcasted_iota(jnp.int32, tile, 1)

    def prepare(n):
        cols = part(n, HD)
        o_cols = pl.ds(pl.multiple_of(f * PAIR + n * HD, HD), HD)
        for t in range(T // TILE):
            rows = part(t, TILE)
            do = do_s[rows, cols]
            qt_s[n, :, rows] = q_ref[rows, cols].T
            dot_s[n, :, rows] = do.T
            delta = jnp.sum(do.astype(f32) * o_ref[rows, o_cols].astype(f32), axis=1, keepdims=True)
            delta_s[n, rows, :] = jnp.broadcast_to(delta, (TILE, HD))
            lse_s[n, rows, :] = jnp.broadcast_to(lse_ref[0, n : n + 1, rows] * (EXP / SCALE), (HD, TILE)).T

    def begin(n, j):
        cols, rows, later = part(n, HD), part(j, TILE), slice(j * TILE, T)
        return dot_t(q_ref[later, cols], k_ref[rows, cols]), dot_t(do_s[later, cols], v_ref[rows, cols])

    def finish(n, j, s, dp):
        cols, rows, later = part(n, HD), part(j, TILE), slice(j * TILE, T)
        twice = lambda ref: jnp.concatenate([ref[n, later, :]] * 2, axis=1)
        p = jnp.exp2(s * EXP - twice(lse_s))
        rest = [p[TILE:]] if p.shape[0] > TILE else []
        p = jnp.concatenate([jnp.where(seen, p[:TILE], 0.0), *rest], axis=0)
        ds = (p * (dp - twice(delta_s))).astype(bf16)
        dv_s[rows, cols] = dot(dot_s[n, :, later], p.astype(bf16)).T.astype(bf16)
        dk = (dot(qt_s[n, :, later], ds) * SCALE).T.astype(bf16).astype(f32)
        dk_s[rows, cols] = turned_back(dk, c_ref[rows, :], s_ref[rows, :])
        dq = dot(ds, k_ref[rows, cols])
        acc_s[n, later, :] = dq + acc_s[n, later, :] if j else dq
        dq = (acc_s[n, rows, :] * SCALE).astype(bf16).astype(f32)
        dq_s[rows, cols] = turned_back(dq, c_ref[rows, :], s_ref[rows, :])

    @pl.when(f < N)
    def _():
        do_s[...] = dot_t(dh1_ref[...], wo_ref[0]).astype(bf16)
        for n in range(2):
            prepare(n)
        todo = [(n, j) for j in range(T // TILE) for n in range(2)]
        ready = [begin(*todo[0])]
        for z, one in enumerate(todo):
            ready += [begin(*two) for two in todo[z + 1 : z + 2]]
            finish(*one, *ready[z])

    red.point(f, sum_ref)

    @pl.when(f < N)
    def _():
        for n, ref in enumerate((dq_s, dk_s, dv_s)):
            red.g[:, :, part(n, BLK), :] = dot(at_s[...], ref[...]).astype(bf16).reshape(4, 2, BLK, PAIR)
        rows = PAIR // N
        piece = gwo_s[:, pl.ds(pl.multiple_of(f * rows, rows), rows), :].reshape(4, 2, rows, D)
        for k in range(2):
            red.g[:, :, part(k, rows, STEPS * BLK), :] = piece[..., part(k, PAIR)]
        red.send(f)
        if need_dh:
            da_s[...] += sum(dot_t(ref[...], w[0]) for ref, w in zip((dq_s, dk_s, dv_s), ws))

    if need_dh:

        @at_step(N - 1)
        def _():
            def end(rows):
                dh_ref[rows, :] = dh1_ref[rows, :] + normed_back(h_ref[rows, :], da_s[rows, :])

            loop(T // TILE, TILE, end)


def attn_bwd(h, dh1, q, k, v, o, lse, wq, wk, wv, wo, c, s, layer):
    need_dh = layer > 0
    win = pl.BlockSpec((1, D, PAIR), lambda i: (layer, 0, clamped(i)))
    col = pl.BlockSpec((T, PAIR), lambda i: (0, clamped(i)))
    lses = pl.BlockSpec((1, 2, T), lambda i: (clamped(i), 0, 0))
    wos = pl.BlockSpec((1, PAIR, D), lambda i: (layer, clamped(i), 0))
    more = int(need_dh)
    return pl.pallas_call(
        functools.partial(attn_bwd_kernel, need_dh=need_dh),
        grid=(N + STEPS,),
        in_specs=[whole(T, D), whole(T, D), col, col, col, whole(T, HH), lses, wos, whole(T, HD), whole(T, HD)] + [win] * (3 * more),
        out_specs=[pl.BlockSpec((1, PAIR, PAIR), lambda i: (summed(i), 0, 0))] + [whole(T, D)] * more,
        out_shape=[shape((N, PAIR, PAIR))] + [shape((T, D))] * more,
        scratch_shapes=[pltpu.VMEM((T, D), f32)] * more
        + [pltpu.VMEM((D, T), bf16)]
        + [pltpu.VMEM((T, PAIR), bf16)] * 4
        + [pltpu.VMEM((2, HD, T), bf16)] * 2
        + [pltpu.VMEM((2, T, HD), f32)] * 3
        + [pltpu.VMEM((N, PAIR, D), bf16)]
        + Reduce.scratch(PAIR, PAIR),
        compiler_params=params(collective_id=3 + layer, has_side_effects=True),
        cost_estimate=cost(16 * T * D * HH + 5 * T * T * HH, T * T * N, N * T * HH),
        name="attn_bwd",
    )(h, dh1, q, k, v, o, lse, wo, c, s, *[wq, wk, wv][: 3 * more])


def adamw(w, m, v, g):
    m = 0.9 * m + 0.1 * g
    v = 0.95 * v + 0.05 * g * g
    return (w - 0.02 * (m * lax.rsqrt(v + 1e-8) + 0.1 * w)).astype(bf16), m, v


def update_kernel(me_ref, sum_ref, *refs, count, before, places):
    del me_ref
    j = pl.program_id(0)
    ws, ms, vs = (refs[i * count : (i + 1) * count] for i in range(3))
    pack_ref, *out = refs[3 * count + before :]
    for i, at, packed, given in places(j):
        own = (0, *at)
        new, m, v = adamw(ws[i][own].astype(f32), ms[i][own], vs[i][own], sum_ref[given].astype(f32))
        pack_ref[packed], out[i][own], out[count + i][own] = new, m, v


def mlp_places(j):
    for n in range(2):
        for f in range(N):
            yield n, (slice(None), part(f, HD)), (part(n, BLK), part(f, HD)), (f, part(n, BLK), pl.ds(pl.multiple_of(j * HD, HD), HD))
    for k in range(2):
        yield 2, (part(k, BLK), slice(None)), (part(2, BLK), part(k, D)), (j, part(2, BLK), part(k, D))


def attn_places(j):
    rows = PAIR // N
    for c in range(2):
        for n in range(3):
            yield n, (slice(None), part(c, PAIR)), (part(n, BLK), part(c, PAIR)), (c, part(n, BLK))
        for k in range(2):
            given = part(k, rows, STEPS * BLK)
            yield STEPS, (part(c, rows), part(k, PAIR)), (given, part(c, PAIR)), (c, given)


def update(me, sums, ws, ms, vs, layer, before):
    count = len(ws)
    if count == 3:
        steps, places = N, mlp_places
        blocks, pack, given = [(BLK, CH), (BLK, CH), (HD, D)], (STEPS * BLK, FF), whole(*sums.shape)
    else:
        steps, places = N // 2, attn_places
        blocks, pack, given = [(BLK, D)] * 4, (PAIR, HH), pl.BlockSpec((2, PAIR, PAIR), lambda j, me: (j, 0, 0))
    own = [pl.BlockSpec((1, *b), lambda j, me: (layer, me[0], j)) for b in blocks[:-1]]
    own += [pl.BlockSpec((1, *blocks[-1]), lambda j, me: (layer, me[0] * steps + j, 0))]
    state = [pl.BlockSpec((1, *b), lambda j, me: (layer, 0, j)) for b in blocks[:-1]]
    state += [pl.BlockSpec((1, *blocks[-1]), lambda j, me: (layer, j, 0))]
    pack_out, *moments = pl.pallas_call(
        functools.partial(update_kernel, count=count, before=len(before), places=places),
        grid_spec=pltpu.PrefetchScalarGridSpec(
            num_scalar_prefetch=1,
            grid=(steps,),
            in_specs=[given, *own, *state, *state] + [HBM] * len(before),
            out_specs=[pl.BlockSpec((pack[0], pack[1] // steps), lambda j, me: (0, j)), *state, *state],
        ),
        out_shape=[shape(pack)] + [shape(a.shape, f32) for a in ms] * 2,
        input_output_aliases={2 + 3 * count + i: 1 + i for i in range(len(before))},
        compiler_params=params(),
        name="update",
    )(me, sums, *ws, *ms, *vs, *before)
    return pack_out, moments


def settle_attn(pack_ref, refs):
    rows = PAIR // N
    for d in range(pack_ref.shape[0] // PAIR):
        base = d * PAIR
        for n in range(3):
            refs[n][0, part(d, BLK)] = pack_ref[part(n, BLK, base), :]
        for i in range(4):
            for c in range(2):
                for k in range(2):
                    refs[3][0, part(2 * i + c, rows, base), part(k, PAIR)] = pack_ref[part(k, rows, base + STEPS * BLK), part(2 * i + c, PAIR)]


def settle_kernel(p0_ref, p1_ref, a1_ref, *refs):
    gate_ref, up_ref, down_ref = refs[4:]
    for layer, pack_ref in enumerate((p0_ref, p1_ref)):
        gate_ref[layer] = pack_ref[part(0, BLK), :]
        up_ref[layer] = pack_ref[part(1, BLK), :]
        for n in range(2 * N):
            down_ref[layer, part(n, BLK)] = pack_ref[part(2, BLK), part(n, D)]
    settle_attn(a1_ref, refs[:4])


def attn_blocks(layer, devices):
    return [pl.BlockSpec((1, devices * BLK, HH), lambda d: (layer, d, 0))] * 3 + [pl.BlockSpec((1, devices * PAIR, D), lambda d: (layer, d, 0))]


def settle(p0, p1, a1):
    mlp = pl.BlockSpec((STEPS * BLK, FF), lambda d: (d, 0))
    tall = lambda r, c: pl.BlockSpec((2, r, c), lambda d: (0, d, 0))
    return pl.pallas_call(
        settle_kernel,
        grid=(N,),
        in_specs=[mlp, mlp, pl.BlockSpec((PAIR, HH), lambda d: (d, 0))],
        out_specs=attn_blocks(1, 1) + [tall(BLK, FF), tall(BLK, FF), tall(CH, D)],
        out_shape=[shape((2, D, HH))] * 3 + [shape((2, HH, D))] + [shape((2, D, FF))] * 2 + [shape((2, FF, D))],
        compiler_params=params(),
        cost_estimate=cost(10**9, 0, 14 * D * FF),
        name="settle",
    )(p0, p1, a1)


def settle_last_kernel(a0_ref, *refs):
    settle_attn(a0_ref, refs[4:])


def settle_last(a0, before):
    return pl.pallas_call(
        settle_last_kernel,
        grid=(2,),
        in_specs=[pl.BlockSpec((4 * PAIR, HH), lambda d: (d, 0))] + [HBM] * 4,
        out_specs=attn_blocks(0, 4),
        out_shape=[shape(b.shape) for b in before],
        input_output_aliases={1 + i: i for i in range(4)},
        compiler_params=params(),
        name="settle_last",
    )(a0, *before)


def solution(mesh):
    def step(x, dy, *arrays):
        weights, m, v = (arrays[i : i + 7] for i in (0, 7, 14))
        wq, wk, wv, wo, wg, wu, wd = weights
        me = lax.axis_index("dp").reshape(1)
        c, s = tables()
        h, kept = x[0], []
        for number in range(2):
            q, k, val, o, lse, h1 = attn_fwd(h, wq, wk, wv, wo, c, s, number)
            kept.append((h, q, k, val, o, lse, h1))
            if number == 0:
                h = mlp_fwd(h1, wg, wu, wd, number)
        dh = dy[0]
        packs, moments = {}, {"mlp": [], "attn": []}
        parts = {"mlp": slice(4, 7), "attn": slice(0, 4)}

        def updated(name, number, sums):
            at = parts[name]
            pack, moments[name] = update(me, sums, weights[at], m[at], v[at], number, moments[name])
            packs[name, number] = lax.all_gather(pack, "dp", axis=0, tiled=True)
            return pack

        for number in (1, 0):
            h, q, k, val, o, lse, h1 = kept[number]
            sums, dh1 = mlp_bwd(h1, dh, wg, wu, wd, number)
            if number == 0:
                sums, packs["attn", 1] = lax.optimization_barrier((sums, packs["attn", 1]))
            pack = updated("mlp", number, sums)
            dh1, _ = lax.optimization_barrier((dh1, pack))
            sums, *rest = attn_bwd(h, dh1, q, k, val, o, lse, wq, wk, wv, wo, c, s, number)
            sums, packs["mlp", number] = lax.optimization_barrier((sums, packs["mlp", number]))
            pack = updated("attn", number, sums)
            if number:
                dh, _ = lax.optimization_barrier((rest[0], pack))
        new = settle(packs["mlp", 0], packs["mlp", 1], packs["attn", 1])
        last = settle_last(packs["attn", 0], new[:4])
        mlp, attn = moments["mlp"], moments["attn"]
        return (*last, *new[4:], *attn[:4], *mlp[:3], *attn[4:], *mlp[3:])

    states, all_of, cut = P(("rep", "dp"), None, None), P(None, None, None), P(None, "dp", None)
    return jax.shard_map(
        step,
        mesh=mesh,
        in_specs=(states, states) + (all_of,) * 7 + (cut,) * 14,
        out_specs=(P("rep", None, None),) * 7 + (P("rep", "dp", None),) * 14,
        check_vma=False,
    )
```

```python
import functools

import jax
import jax.numpy as jnp
from jax import lax
from jax.experimental import pallas as pl
from jax.experimental.pallas import tpu as pltpu
from jax.sharding import PartitionSpec as P

T, D, FF, H, HD = 2048, 512, 8192, 16, 128
N = 8
HH = H * HD
PAIR = 2 * HD
BLK = D // N
CH = FF // N
TILE = 256
KEYS = 512
STEPS = 3
SCALE = HD**-0.5
EXP = SCALE * 1.4426950408889634
EPS = 1e-6
VMEM = 63 * 2**20
f32, bf16 = jnp.float32, jnp.bfloat16
MESH = pl.DeviceIdType.MESH
ONE = pl.Buffered(1)
HBM = pl.BlockSpec(memory_space=pl.ANY)


def dot(a, b):
    return lax.dot_general(a, b, (((1,), (0,)), ((), ())), preferred_element_type=f32)


def dot_t(a, b):
    return lax.dot_general(a, b, (((1,), (1,)), ((), ())), preferred_element_type=f32)


def part(n, size, base=0):
    return slice(base + n * size, base + n * size + size)


def loop(count, size, body):
    lax.fori_loop(0, count, lambda t, _: body(pl.ds(pl.multiple_of(t * size, size), size)), None)


def at_step(n):
    return pl.when(pl.program_id(0) == n)


def normed(h):
    wide = h.astype(f32)
    return (wide * lax.rsqrt(jnp.mean(wide * wide, -1, keepdims=True) + EPS)).astype(bf16)


def normed_back(h, by):
    wide, by = h.astype(f32), by.astype(bf16).astype(f32)
    scale = lax.rsqrt(jnp.mean(wide * wide, -1, keepdims=True) + EPS)
    return (by * scale - wide * (scale * scale * scale * jnp.mean(by * wide, -1, keepdims=True))).astype(bf16)


def turned(x, c, s):
    return (x * c + pltpu.roll(x, HD // 2, 1) * s).astype(bf16)


def turned_back(x, c, s):
    return (x * c - pltpu.roll(x, HD // 2, 1) * s).astype(bf16)


def tables():
    half = HD // 2
    angle = jnp.arange(T, dtype=f32)[:, None] * 10000 ** (-jnp.arange(half, dtype=f32) / half)
    c, s = jnp.cos(angle), jnp.sin(angle)
    return jnp.concatenate([c, c], 1), jnp.concatenate([-s, s], 1)


def whole(*shape):
    return pl.BlockSpec(shape, lambda *_: (0,) * len(shape), pipeline_mode=ONE)


def shape(dims, dtype=bf16):
    return jax.ShapeDtypeStruct(dims, dtype)


def params(**more):
    return pltpu.CompilerParams(dimension_semantics=("arbitrary",), vmem_limit_bytes=VMEM, **more)


def cost(flops, exps, moved):
    return pl.CostEstimate(flops=flops, transcendentals=exps, bytes_accessed=moved)


def attn_fwd_kernel(h_ref, wq_ref, wk_ref, wv_ref, wo_ref, c_ref, s_ref, q_ref, k_ref, v_ref, o_ref, lse_ref, h1_ref, a_s, acc_s, vt_s):
    @at_step(0)
    def _():
        def start(rows):
            a_s[rows, :] = normed(h_ref[rows, :])
            acc_s[rows, :] = jnp.zeros((TILE, D), f32)

        loop(T // TILE, TILE, start)
        vt_s[:, HD:, :] = jnp.ones((2, N, T), bf16)

    wq, wk, wv = wq_ref[0], wk_ref[0], wv_ref[0]
    for t in range(T // KEYS):
        rows = part(t, KEYS)
        a = a_s[rows, :]
        v = dot(a, wv).astype(bf16)
        v_ref[rows, :] = v
        for n in range(2):
            vt_s[n, :HD, rows] = v[:, part(n, HD)].T
        for w, ref in ((wq, q_ref), (wk, k_ref)):
            x = dot(a, w).astype(bf16).astype(f32)
            for n in range(2):
                ref[rows, part(n, HD)] = turned(x[:, part(n, HD)], c_ref[rows, :], s_ref[rows, :])

    tile = (TILE, TILE)
    seen = lax.broadcasted_iota(jnp.int32, tile, 1) >= lax.broadcasted_iota(jnp.int32, tile, 0)

    def scores(n, i):
        cols, rows = part(n, HD), part(i, TILE)
        q = q_ref[rows, cols]
        end = i * TILE
        out = [(a, dot_t(k_ref[a : min(a + KEYS, end), cols], q)) for a in range(0, end, KEYS)]
        return out + [(end, jnp.where(seen, dot_t(k_ref[rows, cols], q), -1e30))]

    def finish(n, i, pieces):
        rows = part(i, TILE)
        top = functools.reduce(jnp.maximum, [s.max(0, keepdims=True) for _, s in pieces])
        mix = sum(dot(vt_s[n, :, a : a + s.shape[0]], jnp.exp2((s - top) * EXP).astype(bf16)) for a, s in pieces)
        total = mix[HD : HD + 1]
        o_ref[rows, part(n, HD)] = (mix[:HD] * (1 / total)).T.astype(bf16)
        lse_ref[0, n : n + 1, rows] = top * SCALE + jnp.log(total)

    todo = [(n, i) for i in range(T // TILE) for n in range(2)]
    ready = [scores(*one) for one in todo[:2]]
    for z, one in enumerate(todo):
        ready += [scores(*two) for two in todo[z + 2 : z + STEPS]]
        finish(*one, ready[z])

    acc_s[...] += dot(o_ref[...], wo_ref[0])

    @at_step(N - 1)
    def _():
        def end(rows):
            h1_ref[rows, :] = h_ref[rows, :] + acc_s[rows, :].astype(bf16)

        loop(T // TILE, TILE, end)


def attn_fwd(h, wq, wk, wv, wo, c, s, layer):
    win = pl.BlockSpec((1, D, PAIR), lambda i: (layer, 0, i))
    col = pl.BlockSpec((T, PAIR), lambda i: (0, i))
    return pl.pallas_call(
        attn_fwd_kernel,
        grid=(N,),
        in_specs=[whole(T, D), win, win, win, pl.BlockSpec((1, PAIR, D), lambda i: (layer, i, 0)), whole(T, HD), whole(T, HD)],
        out_specs=[col] * 4 + [pl.BlockSpec((1, 2, T), lambda i: (i, 0, 0)), whole(T, D)],
        out_shape=[shape((T, HH))] * 4 + [shape((N, 2, T), f32), shape((T, D))],
        scratch_shapes=[pltpu.VMEM((T, D), bf16), pltpu.VMEM((T, D), f32), pltpu.VMEM((2, HD + N, T), bf16)],
        compiler_params=params(),
        cost_estimate=cost(N * T * D * HH + 2 * T * T * HH, T * T * N, N * T * HH),
        name="attn_fwd",
    )(h, wq, wk, wv, wo, c, s)


def mlp_fwd_kernel(h1_ref, wg_ref, wu_ref, wd_ref, h2_ref, b_s, acc_s):
    @at_step(0)
    def _():
        def start(rows):
            b_s[rows, :] = normed(h1_ref[rows, :])
            acc_s[rows, :] = jnp.zeros((TILE, D), f32)

        loop(T // TILE, TILE, start)

    wg, wu, wd = wg_ref[0], wu_ref[0], wd_ref[0]
    for t in range(T // TILE):
        rows = part(t, TILE)
        b = b_s[rows, :]
        gate, up = dot(b, wg), dot(b, wu)
        acc_s[rows, :] += dot((gate / (1 + jnp.exp(-gate)) * up).astype(bf16), wd)

    @at_step(N - 1)
    def _():
        def end(rows):
            h2_ref[rows, :] = h1_ref[rows, :] + acc_s[rows, :].astype(bf16)

        loop(T // TILE, TILE, end)


def mlp_fwd(h1, wg, wu, wd, layer):
    win = pl.BlockSpec((1, D, CH), lambda f: (layer, 0, f))
    return pl.pallas_call(
        mlp_fwd_kernel,
        grid=(N,),
        in_specs=[whole(T, D), win, win, pl.BlockSpec((1, CH, D), lambda f: (layer, f, 0))],
        out_specs=whole(T, D),
        out_shape=shape((T, D)),
        scratch_shapes=[pltpu.VMEM((T, D), bf16), pltpu.VMEM((T, D), f32)],
        compiler_params=params(),
        cost_estimate=cost(6 * T * D * FF, T * FF, 6 * D * FF),
        name="mlp_fwd",
    )(h1, wg, wu, wd)


class Reduce:
    @staticmethod
    def scratch(rows, cols):
        half = (rows, cols // 2)
        return [
            pltpu.VMEM((4, 2, rows, cols), bf16),
            pltpu.VMEM((2, 4, rows, cols), bf16),
            pltpu.VMEM((2, 2, *half), bf16),
            pltpu.VMEM((2, 2, *half), f32),
            pltpu.VMEM((2, 2, 2, *half), bf16),
            pltpu.VMEM((2, *half), bf16),
            pltpu.VMEM((2, *half), f32),
            pltpu.VMEM((2, 2, *half), bf16),
            pltpu.SemaphoreType.DMA((5,)),
            pltpu.SemaphoreType.DMA((2, 5)),
        ]

    def __init__(self, refs):
        self.g, self.r1, self.s2, self.k2, self.r2, self.s3, self.k3, self.r3, self.sent, self.came = refs
        self.rows, self.half = self.s3.shape[1], self.s3.shape[2]
        rep, me = lax.axis_index("rep"), lax.axis_index("dp")
        self.x, self.y, self.c = lax.div(me, 4), lax.rem(lax.div(me, 2), 2), lax.rem(me, 2)
        to = lambda x, y, c: (rep, 4 * x + 2 * y + c)
        self.core = to(self.x, self.y, 1 - self.c)
        self.along = to(1 - self.x, self.y, self.c), to(self.x, 1 - self.y, self.c)

    def enter(self):
        barrier = pltpu.get_barrier_semaphore()
        for one in (self.core, *self.along):
            pl.semaphore_signal(barrier, inc=1, device_id=one, device_id_type=MESH)
        pl.semaphore_wait(barrier, STEPS)

    def copy(self, src, dst, slot, k, device):
        return pltpu.make_async_remote_copy(src, dst, self.sent.at[k], self.came.at[slot, k], device_id=device, device_id_type=MESH)

    def copy1(self, n):
        s = lax.rem(n, 2)
        return self.copy(self.g.at[:, 1 - self.c], self.r1.at[s], s, 0, self.core)

    def copy2(self, n, w):
        s = lax.rem(n, 2)
        return self.copy(self.s2.at[w], self.r2.at[s, w], s, 1 + w, self.along[w])

    def copy3(self, n, w):
        s = lax.rem(n, 2)
        return self.copy(self.s3.at[w], self.r3.at[s, w], s, STEPS + w, self.along[1 - w])

    def run(self, body):
        loop(self.rows // BLK, BLK, body)

    def first(self, n):
        s = lax.rem(n, 2)
        self.copy1(n).wait()
        for w in range(2):
            cols = part(w, self.half)
            for o in range(2):
                away = (2 * (1 - self.x) + o, 2 * o + 1 - self.y)[w]
                near = (2 * self.x + o, 2 * o + self.y)[w]

                def go(r):
                    both = lambda b: self.g[b, self.c, r, cols].astype(f32) + self.r1[s, b, r, cols].astype(f32)
                    self.s2[w, o, r, :] = both(away).astype(bf16)
                    self.k2[w, o, r, :] = both(near)

                self.run(go)
            self.copy2(n, w).start()

    def second(self, n):
        s = lax.rem(n, 2)
        for w in range(2):
            mine = (self.y, self.x)[w]
            self.copy2(n, w).wait()

            def go(r):
                both = lambda b: self.k2[w, b, r, :] + self.r2[s, w, b, r, :].astype(f32)
                self.s3[w, r, :] = both(1 - mine).astype(bf16)
                self.k3[w, r, :] = both(mine)

            self.run(go)
            self.copy3(n, w).start()

    def last(self, n, out_ref):
        s = lax.rem(n, 2)
        for w in range(2):
            self.copy3(n, w).wait()

            def go(r):
                out_ref[0, r, part(w, self.half)] = (self.k3[w, r, :] + self.r3[s, w, r, :].astype(f32)).astype(bf16)

            self.run(go)

    def point(self, f, out_ref):
        for late, stage in ((3, lambda n: self.last(n, out_ref)), (2, self.second), (1, self.first)):
            pl.when((f >= late) & (f < N + late))(functools.partial(stage, f - late))

    def send(self, f):
        self.copy1(f).start()


def mlp_bwd_kernel(*refs):
    h1_ref, dh_ref = refs[:2]
    wgs, wus, refs = refs[2 : 2 + N], refs[2 + N : 2 + 2 * N], refs[2 + 2 * N :]
    wd_ref, wo_ref, o_ref, sum_ref, dh1_ref, do_ref, dwo_ref, b_s, bt_s, dht_s, db_s, wide_s, sems = refs[:13]
    red = Reduce(refs[13:])
    act_s, dg_s, du_s = (wide_s.at[i] for i in range(3))
    f = pl.program_id(0)

    def o_in(half):
        return pltpu.make_async_copy(o_ref.at[:, pl.ds(half * CH, CH)], wide_s.at[half], sems.at[half])

    def do_out(half, t):
        rows = pl.ds(pl.multiple_of(t * KEYS, KEYS), KEYS)
        return pltpu.make_async_copy(wide_s.at[2 - 2 * half, rows], do_ref.at[rows, pl.ds(half * CH, CH)], sems.at[2 + half * (T // KEYS) + t])

    @at_step(0)
    def _():
        red.enter()

        def start(rows):
            b = normed(h1_ref[rows, :])
            b_s[rows, :] = b
            bt_s[:, rows] = b.T
            dht_s[:, rows] = dh_ref[rows, :].T
            db_s[rows, :] = jnp.zeros((TILE, D), f32)

        loop(T // TILE, TILE, start)

    joined = lambda pieces: jnp.concatenate([p[0] for p in pieces], axis=1)

    @pl.when(f < N)
    def _():
        wg, wu, wd = joined(wgs), joined(wus), wd_ref[0].reshape(CH, D)
        for t in range(T // TILE):
            rows = part(t, TILE)
            b = b_s[rows, :]
            gate, up, dact = dot(b, wg), dot(b, wu), dot_t(dh_ref[rows, :], wd).astype(bf16).astype(f32)
            sig = 1 / (1 + jnp.exp(-gate))
            silu = gate * sig
            act_s[rows, :] = (silu * up).astype(bf16)
            du_s[rows, :] = (dact * silu).astype(bf16)
            dg_s[rows, :] = (dact * up * (sig + silu * (1 - sig))).astype(bf16)

    @pl.when(f > N)
    def _():
        half = f - N - 1
        base = half * CH

        def inner(t, _):
            rows = pl.ds(pl.multiple_of(t * KEYS, KEYS), KEYS)
            wide_s[2 - 2 * half, rows, :] = dot_t(dh1_ref[rows, :], wo_ref[0, pl.ds(pl.multiple_of(base, CH), CH), :]).astype(bf16)
            do_out(half, t).start()

        def outer(cols):
            dwo_ref[pl.ds(pl.multiple_of(base + cols.start, TILE), TILE), :] = dot(dht_s[...], wide_s[half, :, cols]).astype(bf16).T

        lax.fori_loop(0, T // KEYS, inner, None)
        o_in(half).wait()
        loop(CH // TILE, TILE, outer)

    red.point(f, sum_ref)

    @at_step(N + 2)
    def _():
        for half in range(2):
            for t in range(T // KEYS):
                do_out(half, t).wait()

    @pl.when(f < N)
    def _():
        for n, ref in enumerate((dg_s, du_s)):
            red.g[:, :, part(n, BLK), :] = dot(bt_s[...], ref[...]).astype(bf16).reshape(4, 2, BLK, CH)
        down = dot(dht_s[...], act_s[...]).astype(bf16).T.reshape(4, 2, HD, D)
        for k in range(2):
            red.g[:, :, part(2, BLK), part(k, D)] = down[:, :, part(k, BLK)]
        red.send(f)
        db_s[...] += dot_t(dg_s[...], joined(wgs)) + dot_t(du_s[...], joined(wus))

    @at_step(N - 1)
    def _():
        o_in(0).start()
        o_in(1).start()

        def end(rows):
            dh1 = dh_ref[rows, :] + normed_back(h1_ref[rows, :], db_s[rows, :])
            dh1_ref[rows, :] = dh1
            dht_s[:, rows] = dh1.T

        loop(T // TILE, TILE, end)


def clamped(i):
    return jnp.minimum(i, N - 1)


def summed(i):
    return jnp.maximum(i - STEPS, 0)


def mlp_bwd(h1, dh, o, wg, wu, wd, wo, layer):
    rows = STEPS * BLK
    cols = [pl.BlockSpec((1, D, HD), functools.partial(lambda d, f: (layer, 0, d * N + clamped(f)), d)) for d in range(N)]
    return pl.pallas_call(
        mlp_bwd_kernel,
        grid=(N + STEPS,),
        in_specs=[whole(T, D), whole(T, D)] + cols * 2
        + [pl.BlockSpec((1, N, HD, D), lambda f: (layer, 0, clamped(f), 0)), pl.BlockSpec((1, HH, D), lambda f: (layer, 0, 0), pipeline_mode=ONE), HBM],
        out_specs=[pl.BlockSpec((1, rows, CH), lambda f: (summed(f), 0, 0)), whole(T, D), HBM, whole(HH, D)],
        out_shape=[shape((N, rows, CH)), shape((T, D)), shape((T, HH)), shape((HH, D))],
        scratch_shapes=[pltpu.VMEM((T, D), bf16), pltpu.VMEM((D, T), bf16), pltpu.VMEM((D, T), bf16), pltpu.VMEM((T, D), f32)]
        + [pltpu.VMEM((3, T, CH), bf16)]
        + [pltpu.SemaphoreType.DMA((2 + 2 * (T // KEYS),))]
        + Reduce.scratch(rows, CH),
        compiler_params=params(collective_id=1 + layer, has_side_effects=True),
        cost_estimate=cost(16 * T * D * FF, T * FF, 12 * D * FF),
        name="mlp_bwd",
    )(h1, dh, *[wg] * N, *[wu] * N, wd.reshape(2, N, CH, D), wo, o)


def attn_bwd_kernel(*refs, need_dh):
    h_ref, q_ref, k_ref, v_ref, o_ref, do_ref, lse_ref, dwo_ref, c_ref, s_ref = refs[:10]
    refs = refs[10:]
    if need_dh:
        ws, dh1_ref, sum_ref, dh_ref, da_s, refs = refs[:3], *refs[3:7], refs[7:]
    else:
        sum_ref, refs = refs[0], refs[1:]
    at_s, dq_s, dk_s, dv_s, qt_s, dot_s, acc_s, lse_s, delta_s = refs[:9]
    red = Reduce(refs[9:])
    f = pl.program_id(0)

    @at_step(0)
    def _():
        red.enter()

        def start(rows):
            at_s[:, rows] = normed(h_ref[rows, :]).T
            if need_dh:
                da_s[rows, :] = jnp.zeros((TILE, D), f32)

        loop(T // TILE, TILE, start)

    tile = (TILE, TILE)
    seen = lax.broadcasted_iota(jnp.int32, tile, 0) >= lax.broadcasted_iota(jnp.int32, tile, 1)

    def prepare(n):
        cols = part(n, HD)
        for t in range(T // TILE):
            rows = part(t, TILE)
            do = do_ref[rows, cols]
            qt_s[n, :, rows] = q_ref[rows, cols].T
            dot_s[n, :, rows] = do.T
            delta = jnp.sum(do.astype(f32) * o_ref[rows, cols].astype(f32), axis=1, keepdims=True)
            delta_s[n, rows, :] = jnp.broadcast_to(delta, (TILE, HD))
            lse_s[n, rows, :] = jnp.broadcast_to(lse_ref[0, n : n + 1, rows] * (EXP / SCALE), (HD, TILE)).T

    def begin(n, j):
        cols, rows, later = part(n, HD), part(j, TILE), slice(j * TILE, T)
        return dot_t(q_ref[later, cols], k_ref[rows, cols]), dot_t(do_ref[later, cols], v_ref[rows, cols])

    def finish(n, j, s, dp):
        cols, rows, later = part(n, HD), part(j, TILE), slice(j * TILE, T)
        twice = lambda ref: jnp.concatenate([ref[n, later, :]] * 2, axis=1)
        p = jnp.exp2(s * EXP - twice(lse_s))
        rest = [p[TILE:]] if p.shape[0] > TILE else []
        p = jnp.concatenate([jnp.where(seen, p[:TILE], 0.0), *rest], axis=0)
        ds = (p * (dp - twice(delta_s))).astype(bf16)
        dv_s[rows, cols] = dot(dot_s[n, :, later], p.astype(bf16)).T.astype(bf16)
        dk = (dot(qt_s[n, :, later], ds) * SCALE).T.astype(bf16).astype(f32)
        dk_s[rows, cols] = turned_back(dk, c_ref[rows, :], s_ref[rows, :])
        dq = dot(ds, k_ref[rows, cols])
        acc_s[n, later, :] = dq + acc_s[n, later, :] if j else dq
        dq = (acc_s[n, rows, :] * SCALE).astype(bf16).astype(f32)
        dq_s[rows, cols] = turned_back(dq, c_ref[rows, :], s_ref[rows, :])

    @pl.when(f < N)
    def _():
        for n in range(2):
            prepare(n)
        todo = [(n, j) for j in range(T // TILE) for n in range(2)]
        ready = [begin(*todo[0])]
        for z, one in enumerate(todo):
            ready += [begin(*two) for two in todo[z + 1 : z + 2]]
            finish(*one, *ready[z])

    red.point(f, sum_ref)

    @pl.when(f < N)
    def _():
        for n, ref in enumerate((dq_s, dk_s, dv_s)):
            red.g[:, :, part(n, BLK), :] = dot(at_s[...], ref[...]).astype(bf16).reshape(4, 2, BLK, PAIR)
        rows = PAIR // N
        piece = dwo_ref[:, pl.ds(pl.multiple_of(f * rows, rows), rows), :].reshape(4, 2, rows, D)
        for k in range(2):
            red.g[:, :, part(k, rows, STEPS * BLK), :] = piece[..., part(k, PAIR)]
        red.send(f)
        if need_dh:
            da_s[...] += sum(dot_t(ref[...], w[0]) for ref, w in zip((dq_s, dk_s, dv_s), ws))

    if need_dh:

        @at_step(N)
        def _():
            def end(rows):
                dh_ref[rows, :] = dh1_ref[rows, :] + normed_back(h_ref[rows, :], da_s[rows, :])

            loop(T // TILE, TILE, end)


def attn_bwd(h, dh1, q, k, v, o, do, lse, wq, wk, wv, dwo, c, s, layer):
    need_dh = layer > 0
    win = pl.BlockSpec((1, D, PAIR), lambda i: (layer, 0, clamped(i)))
    col = pl.BlockSpec((T, PAIR), lambda i: (0, clamped(i)))
    lses = pl.BlockSpec((1, 2, T), lambda i: (clamped(i), 0, 0))
    more = int(need_dh)
    return pl.pallas_call(
        functools.partial(attn_bwd_kernel, need_dh=need_dh),
        grid=(N + STEPS,),
        in_specs=[whole(T, D), col, col, col, col, col, lses, whole(N, PAIR, D), whole(T, HD), whole(T, HD)] + ([win] * 3 + [whole(T, D)]) * more,
        out_specs=[pl.BlockSpec((1, PAIR, PAIR), lambda i: (summed(i), 0, 0))] + [whole(T, D)] * more,
        out_shape=[shape((N, PAIR, PAIR))] + [shape((T, D))] * more,
        scratch_shapes=[pltpu.VMEM((T, D), f32)] * more
        + [pltpu.VMEM((D, T), bf16)]
        + [pltpu.VMEM((T, PAIR), bf16)] * 3
        + [pltpu.VMEM((2, HD, T), bf16)] * 2
        + [pltpu.VMEM((2, T, HD), f32)] * 3
        + Reduce.scratch(PAIR, PAIR),
        compiler_params=params(collective_id=3 + layer, has_side_effects=True),
        cost_estimate=cost(16 * T * D * HH + 5 * T * T * HH, T * T * N, N * T * HH),
        name="attn_bwd",
    )(h, q, k, v, o, do, lse, dwo.reshape(N, PAIR, D), c, s, *[wq, wk, wv, dh1][: 4 * more])


def adamw(w, m, v, g):
    m = 0.9 * m + 0.1 * g
    v = 0.95 * v + 0.05 * g * g
    return (w - 0.02 * (m * lax.rsqrt(v + 1e-8) + 0.1 * w)).astype(bf16), m, v


def update_kernel(me_ref, sum_ref, *refs, count, before, places):
    del me_ref
    j = pl.program_id(0)
    ws, ms, vs = (refs[i * count : (i + 1) * count] for i in range(3))
    pack_ref, *out = refs[3 * count + before :]
    for i, at, packed, given in places(j):
        own = (0, *at)
        new, m, v = adamw(ws[i][own].astype(f32), ms[i][own], vs[i][own], sum_ref[given].astype(f32))
        pack_ref[packed], out[i][own], out[count + i][own] = new, m, v


def mlp_places(j):
    for n in range(2):
        for f in range(N):
            yield n, (slice(None), part(f, HD)), (part(n, BLK), part(f, HD)), (f, part(n, BLK), pl.ds(pl.multiple_of(j * HD, HD), HD))
    for k in range(2):
        yield 2, (part(k, BLK), slice(None)), (part(2, BLK), part(k, D)), (j, part(2, BLK), part(k, D))


def attn_places(j):
    rows = PAIR // N
    for c in range(2):
        for n in range(3):
            yield n, (slice(None), part(c, PAIR)), (part(n, BLK), part(c, PAIR)), (c, part(n, BLK))
        for k in range(2):
            given = part(k, rows, STEPS * BLK)
            yield STEPS, (part(c, rows), part(k, PAIR)), (given, part(c, PAIR)), (c, given)


def update(me, sums, ws, ms, vs, layer, before):
    count = len(ws)
    if count == 3:
        steps, places = N, mlp_places
        blocks, pack, given = [(BLK, CH), (BLK, CH), (HD, D)], (STEPS * BLK, FF), whole(*sums.shape)
    else:
        steps, places = N // 2, attn_places
        blocks, pack, given = [(BLK, D)] * 4, (PAIR, HH), pl.BlockSpec((2, PAIR, PAIR), lambda j, me: (j, 0, 0))
    own = [pl.BlockSpec((1, *b), lambda j, me: (layer, me[0], j)) for b in blocks[:-1]]
    own += [pl.BlockSpec((1, *blocks[-1]), lambda j, me: (layer, me[0] * steps + j, 0))]
    state = [pl.BlockSpec((1, *b), lambda j, me: (layer, 0, j)) for b in blocks[:-1]]
    state += [pl.BlockSpec((1, *blocks[-1]), lambda j, me: (layer, j, 0))]
    pack_out, *moments = pl.pallas_call(
        functools.partial(update_kernel, count=count, before=len(before), places=places),
        grid_spec=pltpu.PrefetchScalarGridSpec(
            num_scalar_prefetch=1,
            grid=(steps,),
            in_specs=[given, *own, *state, *state] + [HBM] * len(before),
            out_specs=[pl.BlockSpec((pack[0], pack[1] // steps), lambda j, me: (0, j)), *state, *state],
        ),
        out_shape=[shape(pack)] + [shape(a.shape, f32) for a in ms] * 2,
        input_output_aliases={2 + 3 * count + i: 1 + i for i in range(len(before))},
        compiler_params=params(),
        name="update",
    )(me, sums, *ws, *ms, *vs, *before)
    return pack_out, moments


def settle_attn(pack_ref, refs):
    rows = PAIR // N
    for d in range(pack_ref.shape[0] // PAIR):
        base = d * PAIR
        for n in range(3):
            refs[n][0, part(d, BLK)] = pack_ref[part(n, BLK, base), :]
        for i in range(4):
            for c in range(2):
                for k in range(2):
                    refs[3][0, part(2 * i + c, rows, base), part(k, PAIR)] = pack_ref[part(k, rows, base + STEPS * BLK), part(2 * i + c, PAIR)]


def settle_kernel(p0_ref, p1_ref, a1_ref, *refs):
    gate_ref, up_ref, down_ref = refs[4:]
    for layer, pack_ref in enumerate((p0_ref, p1_ref)):
        gate_ref[layer] = pack_ref[part(0, BLK), :]
        up_ref[layer] = pack_ref[part(1, BLK), :]
        for n in range(2 * N):
            down_ref[layer, part(n, BLK)] = pack_ref[part(2, BLK), part(n, D)]
    settle_attn(a1_ref, refs[:4])


def attn_blocks(layer, devices):
    return [pl.BlockSpec((1, devices * BLK, HH), lambda d: (layer, d, 0))] * 3 + [pl.BlockSpec((1, devices * PAIR, D), lambda d: (layer, d, 0))]


def settle(p0, p1, a1):
    mlp = pl.BlockSpec((STEPS * BLK, FF), lambda d: (d, 0))
    tall = lambda r, c: pl.BlockSpec((2, r, c), lambda d: (0, d, 0))
    return pl.pallas_call(
        settle_kernel,
        grid=(N,),
        in_specs=[mlp, mlp, pl.BlockSpec((PAIR, HH), lambda d: (d, 0))],
        out_specs=attn_blocks(1, 1) + [tall(BLK, FF), tall(BLK, FF), tall(CH, D)],
        out_shape=[shape((2, D, HH))] * 3 + [shape((2, HH, D))] + [shape((2, D, FF))] * 2 + [shape((2, FF, D))],
        compiler_params=params(),
        cost_estimate=cost(10**9, 0, 14 * D * FF),
        name="settle",
    )(p0, p1, a1)


def settle_last_kernel(a0_ref, *refs):
    settle_attn(a0_ref, refs[4:])


def settle_last(a0, before):
    return pl.pallas_call(
        settle_last_kernel,
        grid=(2,),
        in_specs=[pl.BlockSpec((4 * PAIR, HH), lambda d: (d, 0))] + [HBM] * 4,
        out_specs=attn_blocks(0, 4),
        out_shape=[shape(b.shape) for b in before],
        input_output_aliases={1 + i: i for i in range(4)},
        compiler_params=params(),
        name="settle_last",
    )(a0, *before)


def solution(mesh):
    def step(x, dy, *arrays):
        weights, m, v = (arrays[i : i + 7] for i in (0, 7, 14))
        wq, wk, wv, wo, wg, wu, wd = weights
        me = lax.axis_index("dp").reshape(1)
        c, s = tables()
        h, kept = x[0], []
        for number in range(2):
            q, k, val, o, lse, h1 = attn_fwd(h, wq, wk, wv, wo, c, s, number)
            kept.append((h, q, k, val, o, lse, h1))
            if number == 0:
                h = mlp_fwd(h1, wg, wu, wd, number)
        dh = dy[0]
        packs, moments = {}, {"mlp": [], "attn": []}
        parts = {"mlp": slice(4, 7), "attn": slice(0, 4)}

        def updated(name, number, sums):
            at = parts[name]
            pack, moments[name] = update(me, sums, weights[at], m[at], v[at], number, moments[name])
            if name == "attn":
                pack, packs["mlp", number] = lax.optimization_barrier((pack, packs["mlp", number]))
            packs[name, number] = lax.all_gather(pack, "dp", axis=0, tiled=True)
            return pack

        for number in (1, 0):
            h, q, k, val, o, lse, h1 = kept[number]
            sums, dh1, do, dwo = mlp_bwd(h1, dh, o, wg, wu, wd, wo, number)
            if number == 0:
                sums, packs["attn", 1] = lax.optimization_barrier((sums, packs["attn", 1]))
            pack = updated("mlp", number, sums)
            do, _ = lax.optimization_barrier((do, pack))
            sums, *rest = attn_bwd(h, dh1, q, k, val, o, do, lse, wq, wk, wv, dwo, c, s, number)
            pack = updated("attn", number, sums)
            if number:
                dh, _ = lax.optimization_barrier((rest[0], pack))
        new = settle(packs["mlp", 0], packs["mlp", 1], packs["attn", 1])
        last = settle_last(packs["attn", 0], new[:4])
        mlp, attn = moments["mlp"], moments["attn"]
        return (*last, *new[4:], *attn[:4], *mlp[:3], *attn[4:], *mlp[3:])

    states, all_of, cut = P(("rep", "dp"), None, None), P(None, None, None), P(None, "dp", None)
    return jax.shard_map(
        step,
        mesh=mesh,
        in_specs=(states, states) + (all_of,) * 7 + (cut,) * 14,
        out_specs=(P("rep", None, None),) * 7 + (P("rep", "dp", None),) * 14,
        check_vma=False,
    )
```

```python
import functools

import jax
import jax.numpy as jnp
from jax import lax
from jax.experimental import pallas as pl
from jax.experimental.pallas import tpu as pltpu
from jax.sharding import PartitionSpec as P

T, D, FF, H, HD = 2048, 512, 8192, 16, 128
N = 8
HH = H * HD
PAIR = 2 * HD
BLK = D // N
CH = FF // N
TILE = 256
KEYS = 512
STEPS = 3
SCALE = HD**-0.5
EXP = SCALE * 1.4426950408889634
EPS = 1e-6
VMEM = 63 * 2**20
f32, bf16 = jnp.float32, jnp.bfloat16
MESH = pl.DeviceIdType.MESH
ONE = pl.Buffered(1)
HBM = pl.BlockSpec(memory_space=pl.ANY)


def dot(a, b):
    return lax.dot_general(a, b, (((1,), (0,)), ((), ())), preferred_element_type=f32)


def dot_t(a, b):
    return lax.dot_general(a, b, (((1,), (1,)), ((), ())), preferred_element_type=f32)


def part(n, size, base=0):
    return slice(base + n * size, base + n * size + size)


def loop(count, size, body):
    lax.fori_loop(0, count, lambda t, _: body(pl.ds(pl.multiple_of(t * size, size), size)), None)


def at_step(n):
    return pl.when(pl.program_id(0) == n)


def normed(h):
    wide = h.astype(f32)
    return (wide * lax.rsqrt(jnp.mean(wide * wide, -1, keepdims=True) + EPS)).astype(bf16)


def normed_back(h, by):
    wide, by = h.astype(f32), by.astype(bf16).astype(f32)
    scale = lax.rsqrt(jnp.mean(wide * wide, -1, keepdims=True) + EPS)
    return (by * scale - wide * (scale * scale * scale * jnp.mean(by * wide, -1, keepdims=True))).astype(bf16)


def turned(x, c, s):
    return (x * c + pltpu.roll(x, HD // 2, 1) * s).astype(bf16)


def turned_back(x, c, s):
    return (x * c - pltpu.roll(x, HD // 2, 1) * s).astype(bf16)


def tables():
    half = HD // 2
    angle = jnp.arange(T, dtype=f32)[:, None] * 10000 ** (-jnp.arange(half, dtype=f32) / half)
    c, s = jnp.cos(angle), jnp.sin(angle)
    return jnp.concatenate([c, c], 1), jnp.concatenate([-s, s], 1)


def whole(*shape):
    return pl.BlockSpec(shape, lambda *_: (0,) * len(shape), pipeline_mode=ONE)


def shape(dims, dtype=bf16):
    return jax.ShapeDtypeStruct(dims, dtype)


def params(**more):
    return pltpu.CompilerParams(dimension_semantics=("arbitrary",), vmem_limit_bytes=VMEM, **more)


def cost(flops, exps, moved):
    return pl.CostEstimate(flops=flops, transcendentals=exps, bytes_accessed=moved)


def attn_fwd_kernel(h_ref, wq_ref, wk_ref, wv_ref, wo_ref, c_ref, s_ref, q_ref, k_ref, v_ref, o_ref, lse_ref, h1_ref, a_s, acc_s, vt_s):
    @at_step(0)
    def _():
        def start(rows):
            a_s[rows, :] = normed(h_ref[rows, :])
            acc_s[rows, :] = jnp.zeros((TILE, D), f32)

        loop(T // TILE, TILE, start)
        vt_s[:, HD:, :] = jnp.ones((2, N, T), bf16)

    wq, wk, wv = wq_ref[0], wk_ref[0], wv_ref[0]
    for t in range(T // KEYS):
        rows = part(t, KEYS)
        a = a_s[rows, :]
        v = dot(a, wv).astype(bf16)
        v_ref[rows, :] = v
        for n in range(2):
            vt_s[n, :HD, rows] = v[:, part(n, HD)].T
        for w, ref in ((wq, q_ref), (wk, k_ref)):
            x = dot(a, w).astype(bf16).astype(f32)
            for n in range(2):
                ref[rows, part(n, HD)] = turned(x[:, part(n, HD)], c_ref[rows, :], s_ref[rows, :])

    tile = (TILE, TILE)
    seen = lax.broadcasted_iota(jnp.int32, tile, 1) >= lax.broadcasted_iota(jnp.int32, tile, 0)

    def scores(n, i):
        cols, rows = part(n, HD), part(i, TILE)
        q = q_ref[rows, cols]
        end = i * TILE
        out = [(a, dot_t(k_ref[a : min(a + KEYS, end), cols], q)) for a in range(0, end, KEYS)]
        return out + [(end, jnp.where(seen, dot_t(k_ref[rows, cols], q), -1e30))]

    def finish(n, i, pieces):
        rows = part(i, TILE)
        top = functools.reduce(jnp.maximum, [s.max(0, keepdims=True) for _, s in pieces])
        mix = sum(dot(vt_s[n, :, a : a + s.shape[0]], jnp.exp2((s - top) * EXP).astype(bf16)) for a, s in pieces)
        total = mix[HD : HD + 1]
        o_ref[rows, part(n, HD)] = (mix[:HD] * (1 / total)).T.astype(bf16)
        lse_ref[0, n : n + 1, rows] = top * SCALE + jnp.log(total)

    todo = [(n, i) for i in range(T // TILE) for n in range(2)]
    ready = [scores(*one) for one in todo[:2]]
    for z, one in enumerate(todo):
        ready += [scores(*two) for two in todo[z + 2 : z + STEPS]]
        finish(*one, ready[z])

    acc_s[...] += dot(o_ref[...], wo_ref[0])

    @at_step(N - 1)
    def _():
        def end(rows):
            h1_ref[rows, :] = h_ref[rows, :] + acc_s[rows, :].astype(bf16)

        loop(T // TILE, TILE, end)


def attn_fwd(h, wq, wk, wv, wo, c, s, layer):
    win = pl.BlockSpec((1, D, PAIR), lambda i: (layer, 0, i))
    col = pl.BlockSpec((T, PAIR), lambda i: (0, i))
    return pl.pallas_call(
        attn_fwd_kernel,
        grid=(N,),
        in_specs=[whole(T, D), win, win, win, pl.BlockSpec((1, PAIR, D), lambda i: (layer, i, 0)), whole(T, HD), whole(T, HD)],
        out_specs=[col] * 4 + [pl.BlockSpec((1, 2, T), lambda i: (i, 0, 0)), whole(T, D)],
        out_shape=[shape((T, HH))] * 4 + [shape((N, 2, T), f32), shape((T, D))],
        scratch_shapes=[pltpu.VMEM((T, D), bf16), pltpu.VMEM((T, D), f32), pltpu.VMEM((2, HD + N, T), bf16)],
        compiler_params=params(),
        cost_estimate=cost(N * T * D * HH + 2 * T * T * HH, T * T * N, N * T * HH),
        name="attn_fwd",
    )(h, wq, wk, wv, wo, c, s)


def mlp_fwd_kernel(h1_ref, wg_ref, wu_ref, wd_ref, h2_ref, b_s, acc_s):
    @at_step(0)
    def _():
        def start(rows):
            b_s[rows, :] = normed(h1_ref[rows, :])
            acc_s[rows, :] = jnp.zeros((TILE, D), f32)

        loop(T // TILE, TILE, start)

    wg, wu, wd = wg_ref[0], wu_ref[0], wd_ref[0]
    for t in range(T // TILE):
        rows = part(t, TILE)
        b = b_s[rows, :]
        gate, up = dot(b, wg), dot(b, wu)
        acc_s[rows, :] += dot((gate / (1 + jnp.exp(-gate)) * up).astype(bf16), wd)

    @at_step(N - 1)
    def _():
        def end(rows):
            h2_ref[rows, :] = h1_ref[rows, :] + acc_s[rows, :].astype(bf16)

        loop(T // TILE, TILE, end)


def mlp_fwd(h1, wg, wu, wd, layer):
    win = pl.BlockSpec((1, D, CH), lambda f: (layer, 0, f))
    return pl.pallas_call(
        mlp_fwd_kernel,
        grid=(N,),
        in_specs=[whole(T, D), win, win, pl.BlockSpec((1, CH, D), lambda f: (layer, f, 0))],
        out_specs=whole(T, D),
        out_shape=shape((T, D)),
        scratch_shapes=[pltpu.VMEM((T, D), bf16), pltpu.VMEM((T, D), f32)],
        compiler_params=params(),
        cost_estimate=cost(6 * T * D * FF, T * FF, 6 * D * FF),
        name="mlp_fwd",
    )(h1, wg, wu, wd)


class Reduce:
    @staticmethod
    def scratch(rows, cols):
        half = (rows, cols // 2)
        return [
            pltpu.VMEM((4, 2, rows, cols), bf16),
            pltpu.VMEM((2, 4, rows, cols), bf16),
            pltpu.VMEM((2, 2, *half), bf16),
            pltpu.VMEM((2, 2, *half), f32),
            pltpu.VMEM((2, 2, 2, *half), bf16),
            pltpu.VMEM((2, *half), bf16),
            pltpu.VMEM((2, *half), f32),
            pltpu.VMEM((2, 2, *half), bf16),
            pltpu.SemaphoreType.DMA((5,)),
            pltpu.SemaphoreType.DMA((2, 5)),
        ]

    def __init__(self, refs):
        self.g, self.r1, self.s2, self.k2, self.r2, self.s3, self.k3, self.r3, self.sent, self.came = refs
        self.rows, self.half = self.s3.shape[1], self.s3.shape[2]
        rep, me = lax.axis_index("rep"), lax.axis_index("dp")
        self.x, self.y, self.c = lax.div(me, 4), lax.rem(lax.div(me, 2), 2), lax.rem(me, 2)
        to = lambda x, y, c: (rep, 4 * x + 2 * y + c)
        self.core = to(self.x, self.y, 1 - self.c)
        self.along = to(1 - self.x, self.y, self.c), to(self.x, 1 - self.y, self.c)

    def enter(self):
        barrier = pltpu.get_barrier_semaphore()
        for one in (self.core, *self.along):
            pl.semaphore_signal(barrier, inc=1, device_id=one, device_id_type=MESH)
        pl.semaphore_wait(barrier, STEPS)

    def copy(self, src, dst, slot, k, device):
        return pltpu.make_async_remote_copy(src, dst, self.sent.at[k], self.came.at[slot, k], device_id=device, device_id_type=MESH)

    def copy1(self, n):
        s = lax.rem(n, 2)
        return self.copy(self.g.at[:, 1 - self.c], self.r1.at[s], s, 0, self.core)

    def copy2(self, n, w):
        s = lax.rem(n, 2)
        return self.copy(self.s2.at[w], self.r2.at[s, w], s, 1 + w, self.along[w])

    def copy3(self, n, w):
        s = lax.rem(n, 2)
        return self.copy(self.s3.at[w], self.r3.at[s, w], s, STEPS + w, self.along[1 - w])

    def run(self, body):
        loop(self.rows // BLK, BLK, body)

    def first(self, n):
        s = lax.rem(n, 2)
        self.copy1(n).wait()
        for w in range(2):
            cols = part(w, self.half)
            for o in range(2):
                away = (2 * (1 - self.x) + o, 2 * o + 1 - self.y)[w]
                near = (2 * self.x + o, 2 * o + self.y)[w]

                def go(r):
                    both = lambda b: self.g[b, self.c, r, cols].astype(f32) + self.r1[s, b, r, cols].astype(f32)
                    self.s2[w, o, r, :] = both(away).astype(bf16)
                    self.k2[w, o, r, :] = both(near)

                self.run(go)
            self.copy2(n, w).start()

    def second(self, n):
        s = lax.rem(n, 2)
        for w in range(2):
            mine = (self.y, self.x)[w]
            self.copy2(n, w).wait()

            def go(r):
                both = lambda b: self.k2[w, b, r, :] + self.r2[s, w, b, r, :].astype(f32)
                self.s3[w, r, :] = both(1 - mine).astype(bf16)
                self.k3[w, r, :] = both(mine)

            self.run(go)
            self.copy3(n, w).start()

    def last(self, n, out_ref):
        s = lax.rem(n, 2)
        for w in range(2):
            self.copy3(n, w).wait()

            def go(r):
                out_ref[0, r, part(w, self.half)] = (self.k3[w, r, :] + self.r3[s, w, r, :].astype(f32)).astype(bf16)

            self.run(go)

    def point(self, f, out_ref):
        for late, stage in ((3, lambda n: self.last(n, out_ref)), (2, self.second), (1, self.first)):
            pl.when((f >= late) & (f < N + late))(functools.partial(stage, f - late))

    def send(self, f):
        self.copy1(f).start()


def mlp_bwd_kernel(*refs):
    h1_ref, dh_ref = refs[:2]
    wgs, wus, refs = refs[2 : 2 + N], refs[2 + N : 2 + 2 * N], refs[2 + 2 * N :]
    wd_ref, wo_ref, o_ref, sum_ref, dh1_ref, do_ref, dwo_ref, b_s, bt_s, dht_s, db_s, wide_s, sems = refs[:13]
    red = Reduce(refs[13:])
    act_s, dg_s, du_s = (wide_s.at[i] for i in range(3))
    f = pl.program_id(0)

    def o_in(half):
        return pltpu.make_async_copy(o_ref.at[:, pl.ds(half * CH, CH)], wide_s.at[half], sems.at[half])

    def do_out(half, t):
        rows = pl.ds(pl.multiple_of(t * KEYS, KEYS), KEYS)
        return pltpu.make_async_copy(wide_s.at[2 - 2 * half, rows], do_ref.at[rows, pl.ds(half * CH, CH)], sems.at[2 + half * (T // KEYS) + t])

    @at_step(0)
    def _():
        red.enter()

        def start(rows):
            b = normed(h1_ref[rows, :])
            b_s[rows, :] = b
            bt_s[:, rows] = b.T
            dht_s[:, rows] = dh_ref[rows, :].T
            db_s[rows, :] = jnp.zeros((TILE, D), f32)

        loop(T // TILE, TILE, start)

    joined = lambda pieces: jnp.concatenate([p[0] for p in pieces], axis=1)

    @pl.when(f < N)
    def _():
        wg, wu, wd = joined(wgs), joined(wus), wd_ref[0].reshape(CH, D)
        for t in range(T // TILE):
            rows = part(t, TILE)
            b = b_s[rows, :]
            gate, up, dact = dot(b, wg), dot(b, wu), dot_t(dh_ref[rows, :], wd).astype(bf16).astype(f32)
            sig = 1 / (1 + jnp.exp(-gate))
            silu = gate * sig
            act_s[rows, :] = (silu * up).astype(bf16)
            du_s[rows, :] = (dact * silu).astype(bf16)
            dg_s[rows, :] = (dact * up * (sig + silu * (1 - sig))).astype(bf16)

    @pl.when(f > N)
    def _():
        half = f - N - 1
        base = half * CH

        def inner(t, _):
            rows = pl.ds(pl.multiple_of(t * KEYS, KEYS), KEYS)
            wide_s[2 - 2 * half, rows, :] = dot_t(dh1_ref[rows, :], wo_ref[0, pl.ds(pl.multiple_of(base, CH), CH), :]).astype(bf16)
            do_out(half, t).start()

        def outer(cols):
            dwo_ref[pl.ds(pl.multiple_of(base + cols.start, TILE), TILE), :] = dot(dht_s[...], wide_s[half, :, cols]).astype(bf16).T

        lax.fori_loop(0, T // KEYS, inner, None)
        o_in(half).wait()
        loop(CH // TILE, TILE, outer)

    red.point(f, sum_ref)

    @at_step(N + 2)
    def _():
        for half in range(2):
            for t in range(T // KEYS):
                do_out(half, t).wait()

    @pl.when(f < N)
    def _():
        for n, ref in enumerate((dg_s, du_s)):
            red.g[:, :, part(n, BLK), :] = dot(bt_s[...], ref[...]).astype(bf16).reshape(4, 2, BLK, CH)
        down = dot(dht_s[...], act_s[...]).astype(bf16).T.reshape(4, 2, HD, D)
        for k in range(2):
            red.g[:, :, part(2, BLK), part(k, D)] = down[:, :, part(k, BLK)]
        red.send(f)
        db_s[...] += dot_t(dg_s[...], joined(wgs)) + dot_t(du_s[...], joined(wus))

    @at_step(N - 1)
    def _():
        o_in(0).start()
        o_in(1).start()

        def end(rows):
            dh1 = dh_ref[rows, :] + normed_back(h1_ref[rows, :], db_s[rows, :])
            dh1_ref[rows, :] = dh1
            dht_s[:, rows] = dh1.T

        loop(T // TILE, TILE, end)


def clamped(i):
    return jnp.minimum(i, N - 1)


def summed(i):
    return jnp.maximum(i - STEPS, 0)


def mlp_bwd(h1, dh, o, wg, wu, wd, wo, layer):
    rows = STEPS * BLK
    cols = [pl.BlockSpec((1, D, HD), functools.partial(lambda d, f: (layer, 0, d * N + clamped(f)), d)) for d in range(N)]
    return pl.pallas_call(
        mlp_bwd_kernel,
        grid=(N + STEPS,),
        in_specs=[whole(T, D), whole(T, D)] + cols * 2
        + [pl.BlockSpec((1, N, HD, D), lambda f: (layer, 0, clamped(f), 0)), pl.BlockSpec((1, HH, D), lambda f: (layer, 0, 0), pipeline_mode=ONE), HBM],
        out_specs=[pl.BlockSpec((1, rows, CH), lambda f: (summed(f), 0, 0)), whole(T, D), HBM, whole(HH, D)],
        out_shape=[shape((N, rows, CH)), shape((T, D)), shape((T, HH)), shape((HH, D))],
        scratch_shapes=[pltpu.VMEM((T, D), bf16), pltpu.VMEM((D, T), bf16), pltpu.VMEM((D, T), bf16), pltpu.VMEM((T, D), f32)]
        + [pltpu.VMEM((3, T, CH), bf16)]
        + [pltpu.SemaphoreType.DMA((2 + 2 * (T // KEYS),))]
        + Reduce.scratch(rows, CH),
        compiler_params=params(collective_id=1 + layer, has_side_effects=True),
        cost_estimate=cost(16 * T * D * FF, T * FF, 12 * D * FF),
        name="mlp_bwd",
    )(h1, dh, *[wg] * N, *[wu] * N, wd.reshape(2, N, CH, D), wo, o)


def attn_bwd_kernel(*refs, need_dh):
    h_ref, q_ref, k_ref, v_ref, o_ref, do_ref, lse_ref, dwo_ref, c_ref, s_ref = refs[:10]
    refs = refs[10:]
    if need_dh:
        ws, dh1_ref, sum_ref, dh_ref, da_s, refs = refs[:3], *refs[3:7], refs[7:]
    else:
        sum_ref, refs = refs[0], refs[1:]
    at_s, dq_s, dk_s, dv_s, qt_s, dot_s, acc_s, lse_s, delta_s = refs[:9]
    red = Reduce(refs[9:])
    f = pl.program_id(0)

    @at_step(0)
    def _():
        red.enter()

        def start(rows):
            at_s[:, rows] = normed(h_ref[rows, :]).T
            if need_dh:
                da_s[rows, :] = jnp.zeros((TILE, D), f32)

        loop(T // TILE, TILE, start)

    tile = (TILE, TILE)
    seen = lax.broadcasted_iota(jnp.int32, tile, 0) >= lax.broadcasted_iota(jnp.int32, tile, 1)

    def prepare(n):
        cols = part(n, HD)
        for t in range(T // TILE):
            rows = part(t, TILE)
            do = do_ref[rows, cols]
            qt_s[n, :, rows] = q_ref[rows, cols].T
            dot_s[n, :, rows] = do.T
            delta = jnp.sum(do.astype(f32) * o_ref[rows, cols].astype(f32), axis=1, keepdims=True)
            delta_s[n, rows, :] = jnp.broadcast_to(delta, (TILE, HD))
            lse_s[n, rows, :] = jnp.broadcast_to(lse_ref[0, n : n + 1, rows] * (EXP / SCALE), (HD, TILE)).T

    def begin(n, j):
        cols, rows, later = part(n, HD), part(j, TILE), slice(j * TILE, T)
        return dot_t(q_ref[later, cols], k_ref[rows, cols]), dot_t(do_ref[later, cols], v_ref[rows, cols])

    def finish(n, j, s, dp):
        cols, rows, later = part(n, HD), part(j, TILE), slice(j * TILE, T)
        twice = lambda ref: jnp.concatenate([ref[n, later, :]] * 2, axis=1)
        p = jnp.exp2(s * EXP - twice(lse_s))
        rest = [p[TILE:]] if p.shape[0] > TILE else []
        p = jnp.concatenate([jnp.where(seen, p[:TILE], 0.0), *rest], axis=0)
        ds = (p * (dp - twice(delta_s))).astype(bf16)
        dv_s[rows, cols] = dot(dot_s[n, :, later], p.astype(bf16)).T.astype(bf16)
        dk = (dot(qt_s[n, :, later], ds) * SCALE).T.astype(bf16).astype(f32)
        dk_s[rows, cols] = turned_back(dk, c_ref[rows, :], s_ref[rows, :])
        dq = dot(ds, k_ref[rows, cols])
        acc_s[n, later, :] = dq + acc_s[n, later, :] if j else dq
        dq = (acc_s[n, rows, :] * SCALE).astype(bf16).astype(f32)
        dq_s[rows, cols] = turned_back(dq, c_ref[rows, :], s_ref[rows, :])

    @pl.when(f < N)
    def _():
        for n in range(2):
            prepare(n)
        todo = [(n, j) for j in range(T // TILE) for n in range(2)]
        ready = [begin(*todo[0])]
        for z, one in enumerate(todo):
            ready += [begin(*two) for two in todo[z + 1 : z + 2]]
            finish(*one, *ready[z])

    red.point(f, sum_ref)

    @pl.when(f < N)
    def _():
        for n, ref in enumerate((dq_s, dk_s, dv_s)):
            red.g[:, :, part(n, BLK), :] = dot(at_s[...], ref[...]).astype(bf16).reshape(4, 2, BLK, PAIR)
        rows = PAIR // N
        piece = dwo_ref[:, pl.ds(pl.multiple_of(f * rows, rows), rows), :].reshape(4, 2, rows, D)
        for k in range(2):
            red.g[:, :, part(k, rows, STEPS * BLK), :] = piece[..., part(k, PAIR)]
        red.send(f)
        if need_dh:
            da_s[...] += sum(dot_t(ref[...], w[0]) for ref, w in zip((dq_s, dk_s, dv_s), ws))

    if need_dh:

        @at_step(N)
        def _():
            def end(rows):
                dh_ref[rows, :] = dh1_ref[rows, :] + normed_back(h_ref[rows, :], da_s[rows, :])

            loop(T // TILE, TILE, end)


def attn_bwd(h, dh1, q, k, v, o, do, lse, wq, wk, wv, dwo, c, s, layer):
    need_dh = layer > 0
    win = pl.BlockSpec((1, D, PAIR), lambda i: (layer, 0, clamped(i)))
    col = pl.BlockSpec((T, PAIR), lambda i: (0, clamped(i)))
    lses = pl.BlockSpec((1, 2, T), lambda i: (clamped(i), 0, 0))
    more = int(need_dh)
    return pl.pallas_call(
        functools.partial(attn_bwd_kernel, need_dh=need_dh),
        grid=(N + STEPS,),
        in_specs=[whole(T, D), col, col, col, col, col, lses, whole(N, PAIR, D), whole(T, HD), whole(T, HD)] + ([win] * 3 + [whole(T, D)]) * more,
        out_specs=[pl.BlockSpec((1, PAIR, PAIR), lambda i: (summed(i), 0, 0))] + [whole(T, D)] * more,
        out_shape=[shape((N, PAIR, PAIR))] + [shape((T, D))] * more,
        scratch_shapes=[pltpu.VMEM((T, D), f32)] * more
        + [pltpu.VMEM((D, T), bf16)]
        + [pltpu.VMEM((T, PAIR), bf16)] * 3
        + [pltpu.VMEM((2, HD, T), bf16)] * 2
        + [pltpu.VMEM((2, T, HD), f32)] * 3
        + Reduce.scratch(PAIR, PAIR),
        compiler_params=params(collective_id=3 + layer, has_side_effects=True),
        cost_estimate=cost(16 * T * D * HH + 5 * T * T * HH, T * T * N, N * T * HH),
        name="attn_bwd",
    )(h, q, k, v, o, do, lse, dwo.reshape(N, PAIR, D), c, s, *[wq, wk, wv, dh1][: 4 * more])


def adamw(w, m, v, g):
    m = 0.9 * m + 0.1 * g
    v = 0.95 * v + 0.05 * g * g
    return (w - 0.02 * (m * lax.rsqrt(v + 1e-8) + 0.1 * w)).astype(bf16), m, v


def update_kernel(me_ref, sum_ref, *refs, count, before, places, new_too, moments_too):
    del me_ref
    j = pl.program_id(0)
    ws, ms, vs = (refs[i * count : (i + 1) * count] for i in range(3))
    out = refs[3 * count + before :]
    pack_ref, out = (out[0], out[1:]) if new_too else (None, out)
    for i, at, packed, given in places(j):
        own = (0, *at)
        new, m, v = adamw(ws[i][own].astype(f32), ms[i][own], vs[i][own], sum_ref[given].astype(f32))
        if new_too:
            pack_ref[packed] = new
        if moments_too:
            out[i][own], out[count + i][own] = m, v


def mlp_places(j):
    for n in range(2):
        for f in range(N):
            yield n, (slice(None), part(f, HD)), (part(n, BLK), part(f, HD)), (f, part(n, BLK), pl.ds(pl.multiple_of(j * HD, HD), HD))
    for k in range(2):
        yield 2, (part(k, BLK), slice(None)), (part(2, BLK), part(k, D)), (j, part(2, BLK), part(k, D))


def attn_places(j):
    rows = PAIR // N
    for c in range(2):
        for n in range(3):
            yield n, (slice(None), part(c, PAIR)), (part(n, BLK), part(c, PAIR)), (c, part(n, BLK))
        for k in range(2):
            given = part(k, rows, STEPS * BLK)
            yield STEPS, (part(c, rows), part(k, PAIR)), (given, part(c, PAIR)), (c, given)


def update(me, sums, ws, ms, vs, layer, before, new_too=True, moments_too=True):
    count = len(ws)
    if count == 3:
        steps, places = N, mlp_places
        blocks, pack, given = [(BLK, CH), (BLK, CH), (HD, D)], (STEPS * BLK, FF), whole(*sums.shape)
    else:
        steps, places = N // 2, attn_places
        blocks, pack, given = [(BLK, D)] * 4, (PAIR, HH), pl.BlockSpec((2, PAIR, PAIR), lambda j, me: (j, 0, 0))
    own = [pl.BlockSpec((1, *b), lambda j, me: (layer, me[0], j)) for b in blocks[:-1]]
    own += [pl.BlockSpec((1, *blocks[-1]), lambda j, me: (layer, me[0] * steps + j, 0))]
    state = [pl.BlockSpec((1, *b), lambda j, me: (layer, 0, j)) for b in blocks[:-1]]
    state += [pl.BlockSpec((1, *blocks[-1]), lambda j, me: (layer, j, 0))]
    packs = [pl.BlockSpec((pack[0], pack[1] // steps), lambda j, me: (0, j))] * new_too
    got = pl.pallas_call(
        functools.partial(update_kernel, count=count, before=len(before), places=places, new_too=new_too, moments_too=moments_too),
        grid_spec=pltpu.PrefetchScalarGridSpec(
            num_scalar_prefetch=1,
            grid=(steps,),
            in_specs=[given, *own, *state, *state] + [HBM] * len(before),
            out_specs=packs + [*state, *state] * moments_too,
        ),
        out_shape=[shape(pack)] * new_too + [shape(a.shape, f32) for a in ms] * (2 * moments_too),
        input_output_aliases={2 + 3 * count + i: new_too + i for i in range(len(before))},
        compiler_params=params(),
        cost_estimate=cost(10**9, 0, 10 * D * FF),
        name="update",
    )(me, sums, *ws, *ms, *vs, *before)
    return (got[0] if new_too else None), list(got[new_too:])


def settle_attn(pack_ref, refs):
    rows = PAIR // N
    for d in range(pack_ref.shape[0] // PAIR):
        base = d * PAIR
        for n in range(3):
            refs[n][0, part(d, BLK)] = pack_ref[part(n, BLK, base), :]
        for i in range(4):
            for c in range(2):
                for k in range(2):
                    refs[3][0, part(2 * i + c, rows, base), part(k, PAIR)] = pack_ref[part(k, rows, base + STEPS * BLK), part(2 * i + c, PAIR)]


def settle_kernel(p0_ref, p1_ref, a1_ref, *refs):
    gate_ref, up_ref, down_ref = refs[4:]
    for layer, pack_ref in enumerate((p0_ref, p1_ref)):
        gate_ref[layer] = pack_ref[part(0, BLK), :]
        up_ref[layer] = pack_ref[part(1, BLK), :]
        for n in range(2 * N):
            down_ref[layer, part(n, BLK)] = pack_ref[part(2, BLK), part(n, D)]
    settle_attn(a1_ref, refs[:4])


def attn_blocks(layer, devices):
    return [pl.BlockSpec((1, devices * BLK, HH), lambda d: (layer, d, 0))] * 3 + [pl.BlockSpec((1, devices * PAIR, D), lambda d: (layer, d, 0))]


def settle(p0, p1, a1):
    mlp = pl.BlockSpec((STEPS * BLK, FF), lambda d: (d, 0))
    tall = lambda r, c: pl.BlockSpec((2, r, c), lambda d: (0, d, 0))
    return pl.pallas_call(
        settle_kernel,
        grid=(N,),
        in_specs=[mlp, mlp, pl.BlockSpec((PAIR, HH), lambda d: (d, 0))],
        out_specs=attn_blocks(1, 1) + [tall(BLK, FF), tall(BLK, FF), tall(CH, D)],
        out_shape=[shape((2, D, HH))] * 3 + [shape((2, HH, D))] + [shape((2, D, FF))] * 2 + [shape((2, FF, D))],
        compiler_params=params(),
        cost_estimate=cost(10**9, 0, 14 * D * FF),
        name="settle",
    )(p0, p1, a1)


def settle_last_kernel(a0_ref, *refs):
    settle_attn(a0_ref, refs[4:])


def settle_last(a0, before):
    return pl.pallas_call(
        settle_last_kernel,
        grid=(2,),
        in_specs=[pl.BlockSpec((4 * PAIR, HH), lambda d: (d, 0))] + [HBM] * 4,
        out_specs=attn_blocks(0, 4),
        out_shape=[shape(b.shape) for b in before],
        input_output_aliases={1 + i: i for i in range(4)},
        compiler_params=params(),
        name="settle_last",
    )(a0, *before)


def solution(mesh):
    def step(x, dy, *arrays):
        weights, m, v = (arrays[i : i + 7] for i in (0, 7, 14))
        wq, wk, wv, wo, wg, wu, wd = weights
        me = lax.axis_index("dp").reshape(1)
        c, s = tables()
        h, kept = x[0], []
        for number in range(2):
            q, k, val, o, lse, h1 = attn_fwd(h, wq, wk, wv, wo, c, s, number)
            kept.append((h, q, k, val, o, lse, h1))
            if number == 0:
                h = mlp_fwd(h1, wg, wu, wd, number)
        dh = dy[0]
        packs, moments, later = {}, {"mlp": [], "attn": []}, {}
        parts = {"mlp": slice(4, 7), "attn": slice(0, 4)}

        def updated(name, number, sums):
            at = parts[name]
            given = me, sums, weights[at], m[at], v[at], number
            if number or name == "attn":
                pack, moments[name] = update(*given, moments[name])
            else:
                pack, _ = update(*given, [], moments_too=False)
                later[name] = given
            if name == "attn":
                pack, packs["mlp", number] = lax.optimization_barrier((pack, packs["mlp", number]))
            packs[name, number] = lax.all_gather(pack, "dp", axis=0, tiled=True)
            return pack

        for number in (1, 0):
            h, q, k, val, o, lse, h1 = kept[number]
            sums, dh1, do, dwo = mlp_bwd(h1, dh, o, wg, wu, wd, wo, number)
            if number == 0:
                sums, packs["attn", 1] = lax.optimization_barrier((sums, packs["attn", 1]))
            pack = updated("mlp", number, sums)
            do, _ = lax.optimization_barrier((do, pack))
            sums, *rest = attn_bwd(h, dh1, q, k, val, o, do, lse, wq, wk, wv, dwo, c, s, number)
            pack = updated("attn", number, sums)
            if number:
                dh, _ = lax.optimization_barrier((rest[0], pack))
        for name, (me, sums, *given) in later.items():
            sums, _ = lax.optimization_barrier((sums, pack))
            _, moments[name] = update(me, sums, *given, moments[name], new_too=False)
        new = settle(packs["mlp", 0], packs["mlp", 1], packs["attn", 1])
        last = settle_last(packs["attn", 0], new[:4])
        mlp, attn = moments["mlp"], moments["attn"]
        return (*last, *new[4:], *attn[:4], *mlp[:3], *attn[4:], *mlp[3:])

    states, all_of, cut = P(("rep", "dp"), None, None), P(None, None, None), P(None, "dp", None)
    return jax.shard_map(
        step,
        mesh=mesh,
        in_specs=(states, states) + (all_of,) * 7 + (cut,) * 14,
        out_specs=(P("rep", None, None),) * 7 + (P("rep", "dp", None),) * 14,
        check_vma=False,
    )
```
